32 devices in a mesh: parts: 2 (over y), gz: 8 (over z, x), gy: 2 (over core).
Axes of the slice: x: 2, y: 2, z: 4, core: 2. Of those that a mesh axis runs over, the one named last changes fastest.
Arguments:
- direction: float32 [3, 16, 128, 128], P(None, ('parts', 'gz'), 'gy'), parts along dimension 1, may hold values from -6 to 6
- region: int32 [16, 128, 128], P(('parts', 'gz'), 'gy'), parts along dimension 0, may hold values from 0 to 3
- saturation: float32 [3], replicated, may hold values from 0.5 to 2
- kernel_main: float32 [6, 16, 256, 128], P(None, 'gz', 'gy'), may hold values from -6 to 6
- kernel_nyq: float32 [6, 16, 256], P(None, 'gz', 'gy'), may hold values from -6 to 6
Outputs:
- field: float32 [3, 16, 128, 128], P(None, ('parts', 'gz'), 'gy'), parts along dimension 1
The draws below stay inside these ranges and needn't reach their ends.
There are 2 independent parts, one for each index of `parts`. The reference program is written for one: setup_inputs(seed, part) draws one part's arguments, and reference() takes and returns one part's arrays. A program takes and returns all parts, laid end to end along the dimension named above; an argument that names none is the same for every part. Nothing has to cross between parts.
Inputs may be any that keep to these rules, and one draw needn't show every extreme that they name: `region`: 0 marks an empty cell; other ids name materials.
All inputs are finite; a program needn't handle non-finite values.
Results may differ from the reference program's by a relative error of at most 0.00007.
Values sent between devices are 32-bit elements; how exact they have to be, the bound alone decides.
A program may use at most 64 MiB of HBM per device.

```python
import math
import jax
import jax.numpy as jnp
import numpy as np

MX = 128
MY = 128
REGIONS = 4
MZ = 8
PY = 256
PZ = 16
ZBITS = 3


def touch_ends(array, key, smallest, largest):
    place = [jax.random.randint(jax.random.fold_in(key, axis), (), 0, length) for axis, length in enumerate(array.shape)]
    longest = array.shape.index(max(array.shape))
    neighbour = place[:longest] + [(place[longest] + 1) % array.shape[longest]] + place[longest + 1:]
    return array.at[tuple(place)].set(smallest).at[tuple(neighbour)].set(largest)


def level_of(own_key, dims, cuts, least, high):
    loudness, own = 1.0, jax.random.fold_in(own_key, 6)
    for dim, shards_of in cuts:
        draws = jnp.exp(jax.random.uniform(jax.random.fold_in(own, dim), (shards_of,), jnp.float32, least / len(cuts), high / len(cuts)))
        loudness = loudness * jnp.repeat(draws, dims[dim] // shards_of).reshape([-1 if axis == dim else 1 for axis in range(len(dims))])
    return loudness


def noise(rng, extent, deviation, reach, cuts=(), dtype=jnp.bfloat16):
    entries = jax.random.normal(rng, extent, jnp.float32) * deviation
    if len(cuts) > 0:
        entries = level_of(rng, extent, cuts, -0.22, 0.18) * entries
    return jnp.clip(entries, min=-reach, max=reach).astype(dtype)


def setup_inputs(seed: int = 0, part: int = 0) -> dict:
    seeds = jax.random.split(jax.random.key(seed), 6)
    part_keys = jax.random.split(jax.random.fold_in(seeds[5], part), 6)
    return {
        "direction": noise(part_keys[0], (3, MZ, MY, MX), 1.0, 6.0, ((1, 8), (2, 2)), jnp.float32),
        "region": touch_ends(jax.random.randint(part_keys[1], (MZ, MY, MX), 0, REGIONS), jax.random.fold_in(part_keys[1], 1), 0, REGIONS - 1).astype(jnp.int32),
        "saturation": jnp.clip(jnp.exp(jax.random.uniform(seeds[2], (REGIONS - 1,), jnp.float32, math.log(0.5), math.log(2.0))), 0.5, 2.0),
        "kernel_main": noise(seeds[3], (6, PZ, PY, MX), 1.0, 6.0, ((1, 8), (2, 2)), jnp.float32),
        "kernel_nyq": noise(seeds[4], (6, PZ, PY), 1.0, 6.0, ((1, 8), (2, 2)), jnp.float32),
    }


exchange_stiffness = 0.25
tensor_index = ((0, 3, 4), (3, 1, 5), (4, 5, 2))


def slot_order(bit_count):
    slot_index = np.arange(2 ** (bit_count + 1))
    device = slot_index // 2
    reversed_bits = device * 0
    for b in range(bit_count):
        reversed_bits = reversed_bits + ((device >> b) & 1) * (2 ** (bit_count - 1 - b))
    return 2 * reversed_bits + slot_index % 2


def neighbours(padded):
    summed = padded[..., 2:, 1:-1, 1:-1] + padded[..., :-2, 1:-1, 1:-1]
    summed = summed + padded[..., 1:-1, 2:, 1:-1] + padded[..., 1:-1, :-2, 1:-1]
    return summed + padded[..., 1:-1, 1:-1, 2:] + padded[..., 1:-1, 1:-1, :-2]


def reference(direction, region, saturation, kernel_main, kernel_nyq):
    magnetic = (region > 0).astype(jnp.float32)
    strength = jnp.zeros(region.shape, jnp.float32)
    for r in range(REGIONS - 1):
        strength = strength + jnp.where(region == r + 1, saturation[r], 0.0)
    moment = direction * strength[None]
    padded = jnp.zeros((3, 2 * MZ, 2 * MY, 2 * MX), jnp.float32).at[:, :MZ, :MY, :MX].set(moment)
    spectra = jnp.fft.rfftn(padded, axes=(1, 2, 3))
    inverse_slots = np.argsort(slot_order(ZBITS)).astype(np.int32)
    kernel = jnp.concatenate([kernel_main, kernel_nyq[..., None]], axis=3)[:, inverse_slots]
    pieces = []
    for i in range(3):
        summed = kernel[tensor_index[i][0]] * spectra[0]
        for j in (1, 2):
            summed = summed + kernel[tensor_index[i][j]] * spectra[j]
        pieces.append(summed)
    demag = jnp.fft.irfftn(jnp.stack(pieces), s=(2 * MZ, 2 * MY, 2 * MX), axes=(1, 2, 3))
    demag = demag[:, :MZ, :MY, :MX]
    moment_rim = jnp.pad(direction * magnetic[None], ((0, 0), (1, 1), (1, 1), (1, 1)))
    count_rim = jnp.pad(magnetic, 1)
    near = neighbours(moment_rim)
    count = neighbours(count_rim)
    exchange = exchange_stiffness * magnetic[None] * (near - count[None] * direction)
    return (demag + exchange).astype(jnp.float32)
```

```python
import functools
import math

import jax
import jax.numpy as jnp
import numpy as np
from jax import lax
from jax.experimental import pallas as pl
from jax.experimental.pallas import tpu as pltpu
from jax.sharding import PartitionSpec as P

exchange_stiffness = 0.25
tensor_index = ((0, 3, 4), (3, 1, 5), (4, 5, 2))
highest = lax.Precision.HIGHEST


def with_halo(cells, sides, width):
    for axis, dim in sides:
        count = lax.axis_size(axis)
        ends = count - 1
        head = lax.slice_in_dim(cells, 0, width, axis=dim)
        tail = lax.slice_in_dim(cells, cells.shape[dim] - width, cells.shape[dim], axis=dim)
        cells = jnp.concatenate(
            [
                lax.ppermute(tail, axis, [(i, (i + 1) % count) for i in range(ends)]),
                cells,
                lax.ppermute(head, axis, [((i + 1) % count, i) for i in range(ends)]),
            ],
            axis=dim,
        )
    return cells


def phase(first, second, period):
    product = first[:, None] * second[None, :] % period
    angle = 2.0 * math.pi / period * product.astype(jnp.float32)
    return (jnp.cos(angle), jnp.sin(angle))


def slot_frequency(slot_index, bit_count):
    device = slot_index // 2
    reversed_bits = jnp.zeros_like(device)
    for b in range(bit_count):
        reversed_bits = reversed_bits + device // 2**b % 2 * 2 ** (bit_count - 1 - b)
    return 2 * reversed_bits + slot_index % 2


def row_transform(plane):
    columns = plane.shape[2]
    row_count = plane.shape[1]
    positions = jnp.arange(columns, dtype=jnp.int32)
    cosine, sine = phase(positions, positions, 2 * columns)
    table = jnp.concatenate([cosine, -sine], axis=1)
    flat = plane.reshape(3 * row_count, columns)
    both = jnp.dot(flat, table, precision=highest).reshape(3, row_count, 2, columns)
    signs = 1.0 - 2.0 * (positions % 2).astype(jnp.float32)
    nyquist = jnp.dot(flat, signs, precision=highest).reshape(3, row_count)
    return (both[:, :, 0], both[:, :, 1], nyquist)


def column_transform(real_rows, imag_rows, nyquist, cosine, sine):
    new_real = jnp.einsum("kr,crx->ckx", cosine, real_rows, precision=highest) + jnp.einsum(
        "kr,crx->ckx", sine, imag_rows, precision=highest
    )
    new_imag = jnp.einsum("kr,crx->ckx", cosine, imag_rows, precision=highest) - jnp.einsum(
        "kr,crx->ckx", sine, real_rows, precision=highest
    )
    nyq_real = jnp.einsum("kr,cr->ck", cosine, nyquist, precision=highest)
    nyq_imag = -jnp.einsum("kr,cr->ck", sine, nyquist, precision=highest)
    return (jnp.stack([new_real, new_imag], axis=1), jnp.stack([nyq_real, nyq_imag], axis=1))


def plane_transform(values, cosine, sine, direction_sign):
    real_part = values[:, 0]
    imag_part = values[:, 1]
    new_real = jnp.einsum(
        "pz,cz...->cp...", cosine, real_part, precision=highest
    ) - direction_sign * jnp.einsum("pz,cz...->cp...", sine, imag_part, precision=highest)
    new_imag = jnp.einsum(
        "pz,cz...->cp...", cosine, imag_part, precision=highest
    ) + direction_sign * jnp.einsum("pz,cz...->cp...", sine, real_part, precision=highest)
    return jnp.stack([new_real, new_imag], axis=1)


def apply_kernel(spectra, kernel):
    pieces = []
    for i in range(3):
        summed = kernel[tensor_index[i][0]] * spectra[0]
        for j in (1, 2):
            summed = summed + kernel[tensor_index[i][j]] * spectra[j]
        pieces.append(summed)
    return jnp.stack(pieces)


def local(direction, region, saturation, kernel_main, kernel_nyq):
    columns = direction.shape[3]
    own_rows = direction.shape[2]
    groups_y = lax.axis_size("gy")
    groups_z = lax.axis_size("gz")
    bit_count = groups_z.bit_length() - 1
    rows_total = own_rows * groups_y
    period_y = 2 * rows_total
    period_z = 2 * groups_z
    period_x = 2 * columns
    spec_rows = period_y // groups_y
    y_index = lax.axis_index("gy")
    magnetic = (region > 0).astype(jnp.float32)
    strength = jnp.zeros(region.shape, jnp.float32)
    for r in range(saturation.shape[0]):
        strength = strength + jnp.where(region == r + 1, saturation[r], 0.0)
    magnet_plane = (direction * strength[None])[:, 0]
    gathered = lax.all_gather(magnet_plane, "gy", axis=1, tiled=True)
    frequency = y_index * spec_rows + jnp.arange(spec_rows, dtype=jnp.int32)
    cosine, sine = phase(frequency, jnp.arange(rows_total, dtype=jnp.int32), period_y)
    real_rows, imag_rows, nyquist = row_transform(gathered)
    spec_main, spec_nyq = column_transform(real_rows, imag_rows, nyquist, cosine, sine)
    slot_freq = slot_frequency(jnp.arange(period_z, dtype=jnp.int32), bit_count)
    plane_ids = jnp.arange(groups_z, dtype=jnp.int32)
    sent_main, sent_nyq = (
        lax.all_to_all(spec_main[:, :, None], "gz", split_axis=3, concat_axis=2, tiled=True),
        lax.all_to_all(spec_nyq[:, :, None], "gz", split_axis=3, concat_axis=2, tiled=True),
    )
    cosine, sine = phase(slot_freq, plane_ids, period_z)
    done_main = plane_transform(sent_main, cosine, sine, -1.0)
    done_nyq = plane_transform(sent_nyq, cosine, sine, -1.0)
    full_main, full_nyq = (
        lax.all_to_all(done_main, "gz", split_axis=2, concat_axis=3, tiled=True),
        lax.all_to_all(done_nyq, "gz", split_axis=2, concat_axis=3, tiled=True),
    )
    field_main = apply_kernel(full_main, kernel_main)
    field_nyq = apply_kernel(full_nyq, kernel_nyq)
    out_main, out_nyq = (
        lax.all_to_all(field_main, "gz", split_axis=3, concat_axis=2, tiled=True),
        lax.all_to_all(field_nyq, "gz", split_axis=3, concat_axis=2, tiled=True),
    )
    cosine, sine = phase(plane_ids, slot_freq, period_z)
    back_main = plane_transform(out_main, cosine, sine, 1.0)
    back_nyq = plane_transform(out_nyq, cosine, sine, 1.0)
    plane_main, plane_nyq = (
        lax.all_to_all(back_main, "gz", split_axis=2, concat_axis=3, tiled=True),
        lax.all_to_all(back_nyq, "gz", split_axis=2, concat_axis=3, tiled=True),
    )
    plane_main = plane_main[:, :, 0]
    plane_nyq = plane_nyq[:, :, 0]
    frequency = y_index * spec_rows + jnp.arange(spec_rows, dtype=jnp.int32)
    cosine, sine = phase(jnp.arange(rows_total, dtype=jnp.int32), frequency, period_y)
    term_real = jnp.einsum("yk,ckx->cyx", cosine, plane_main[:, 0], precision=highest) - jnp.einsum(
        "yk,ckx->cyx", sine, plane_main[:, 1], precision=highest
    )
    term_imag = jnp.einsum("yk,ckx->cyx", cosine, plane_main[:, 1], precision=highest) + jnp.einsum(
        "yk,ckx->cyx", sine, plane_main[:, 0], precision=highest
    )
    nyq_real = jnp.einsum("yk,ck->cy", cosine, plane_nyq[:, 0], precision=highest) - jnp.einsum(
        "yk,ck->cy", sine, plane_nyq[:, 1], precision=highest
    )
    nyq_imag = jnp.einsum("yk,ck->cy", cosine, plane_nyq[:, 1], precision=highest) + jnp.einsum(
        "yk,ck->cy", sine, plane_nyq[:, 0], precision=highest
    )
    rows_main, rows_nyq = (
        lax.psum_scatter(
            jnp.stack([term_real, term_imag], axis=1), "gy", scatter_dimension=2, tiled=True
        ),
        lax.psum_scatter(
            jnp.stack([nyq_real, nyq_imag], axis=1), "gy", scatter_dimension=2, tiled=True
        ),
    )
    positions = jnp.arange(columns, dtype=jnp.int32)
    cosine, sine = phase(positions, positions, period_x)
    weights = jnp.where(positions == 0, 1.0, 2.0).astype(jnp.float32)[:, None]
    table = jnp.concatenate([weights * cosine, -weights * sine], axis=0)
    flat = jnp.concatenate([rows_main[:, 0], rows_main[:, 1]], axis=2).reshape(
        3 * own_rows, 2 * columns
    )
    signs = 1.0 - 2.0 * (positions % 2).astype(jnp.float32)
    demag = jnp.dot(flat, table, precision=highest).reshape(3, own_rows, columns)
    demag = demag + rows_nyq[:, 0][:, :, None] * signs[None, None, :]
    demag = demag * (1.0 / (period_x * period_y * period_z))
    moment = direction * magnetic[None]
    stacked = jnp.concatenate([moment, magnetic[None]], axis=0)
    rim = with_halo(stacked, (("gz", 1), ("gy", 2)), 1)
    centre = rim[:, 1:2, 1:-1]
    near = rim[:, 0:1, 1:-1] + rim[:, 2:3, 1:-1] + rim[:, 1:2, :-2] + rim[:, 1:2, 2:]
    padded_x = jnp.pad(centre, ((0, 0), (0, 0), (0, 0), (1, 1)))
    near = near + padded_x[..., :-2] + padded_x[..., 2:]
    exchange = exchange_stiffness * magnetic[None] * (near[:3] - near[3:4] * direction)
    return demag[:, None] + exchange


MESH = pl.DeviceIdType.MESH
most_unrolled_planes = 16


def halves(table):
    high = table.astype(np.float32).astype(jnp.bfloat16)
    low = (table - high.astype(np.float64)).astype(np.float32).astype(jnp.bfloat16)
    return np.stack([high, low])


@functools.lru_cache(maxsize=None)
def tables(columns, rows_total, groups_y, groups_z):
    x = np.arange(columns)
    ang = np.pi / columns * (np.outer(x, x) % (2 * columns))
    c, s = np.cos(ang), np.sin(ang)
    fwd = np.block([[c, -s], [s, c]])
    w = np.where(x == 0, 1.0, 2.0)[:, None]
    inv = np.block([[w * c, w * s], [-w * s, w * c]])
    tx = np.stack([halves(fwd), halves(inv)])
    spec = 2 * rows_total // groups_y
    y = np.arange(rows_total)
    ty = []
    for g in range(groups_y):
        ky = g * spec + np.arange(spec)
        ang = np.pi / rows_total * (np.outer(ky, y) % (2 * rows_total))
        c, s = np.cos(ang), np.sin(ang)
        f = np.block([[c, s], [-s, c]])
        ty.append(np.stack([halves(f), halves(f.T)]))
    ty = np.stack(ty)
    signs = 1.0 - 2.0 * (x % 2)
    gather = np.zeros((6 * columns, columns))
    spread = np.zeros((columns, 6 * columns))
    for b in range(6):
        gather[b * columns : (b + 1) * columns, b] = signs
        gather[b * columns : (b + 1) * columns, b + 6] = signs
        spread[b, b * columns : (b + 1) * columns] = signs
    pick = np.zeros((3, 12, columns))
    for d in range(3):
        for i in range(3):
            for k in range(2):
                pick[d, tensor_index[i][(i + d) % 3] * 2 + k, i * 2 + k] = 1.0
    bits = groups_z.bit_length() - 1
    coef = np.zeros((groups_z, 4 * groups_z))
    plane = np.arange(groups_z)
    for g in range(groups_z):
        rev = sum(((g >> b) & 1) << (bits - 1 - b) for b in range(bits))
        for k in range(2):
            ang = np.pi / groups_z * ((2 * rev + k) * plane % (2 * groups_z))
            coef[g, 2 * k :: 4] = np.cos(ang)
            coef[g, 2 * k + 1 :: 4] = -np.sin(ang)
    return (
        tx,
        ty,
        gather.astype(jnp.bfloat16),
        spread.astype(jnp.bfloat16),
        pick.astype(np.float32),
        coef.astype(np.float32),
    )


def split(value):
    high = value.astype(jnp.bfloat16)
    return high, (value - high.astype(jnp.float32)).astype(jnp.bfloat16)


def mm(a, b):
    return jnp.dot(a, b, preferred_element_type=jnp.float32)


def fused(
    coef,
    sat,
    direction,
    region,
    pick,
    knyq,
    kmain_hbm,
    tx_hbm,
    ty_hbm,
    gather_hbm,
    spread_hbm,
    out,
    mom,
    strength,
    near_strength,
    exch,
    kmain,
    tx,
    ty,
    gather,
    spread,
    zh,
    zl,
    rh,
    rl,
    gh,
    gl,
    afull,
    apeer,
    xsend,
    xrecv,
    upsend,
    uprecv,
    dnsend,
    dnrecv,
    local_sem,
    ag_send,
    ag_ici,
    ag_d2d,
    s_send,
    s_recv,
    a_send,
    a_recv,
    x_ssem,
    x_rsem,
    up_ssem,
    up_rsem,
    dn_ssem,
    dn_rsem,
):
    planes = mom.shape[0]
    line = planes // 2
    rows_total = mom.shape[2]
    columns = mom.shape[3]
    rows = direction.shape[2]
    g = lax.axis_index("gz")
    c = lax.axis_index("gy")
    o = g // 2
    xi = g % 2
    side = g + 1 - 2 * xi
    own = pl.ds(pl.multiple_of(c * rows, rows), rows)
    other = pl.ds(pl.multiple_of((1 - c) * rows, rows), rows)
    peer_id = {"gz": g, "gy": 1 - c}
    side_id = {"gz": side, "gy": c}
    up_id = {"gz": g + 2, "gy": c}
    dn_id = {"gz": g - 2, "gy": c}
    after_id = {"gz": g + 1, "gy": c}
    before_id = {"gz": g - 1, "gy": c}
    has_up = o < line - 1
    has_dn = o > 0
    has_after = g < planes - 1
    has_before = g > 0

    barrier = pltpu.get_barrier_semaphore()
    pl.semaphore_signal(barrier, inc=1, device_id=peer_id, device_id_type=MESH)
    pl.semaphore_signal(barrier, inc=1, device_id=side_id, device_id_type=MESH)
    for cond, where in ((has_up, up_id), (has_dn, dn_id), (has_after, after_id), (has_before, before_id)):

        @pl.when(cond)
        def _(where=where):
            pl.semaphore_signal(barrier, inc=1, device_id=where, device_id_type=MESH)

    loads = [
        pltpu.make_async_copy(kmain_hbm, kmain, local_sem.at[0]),
        pltpu.make_async_copy(tx_hbm, tx, local_sem.at[1]),
        pltpu.make_async_copy(ty_hbm.at[c], ty, local_sem.at[2]),
        pltpu.make_async_copy(gather_hbm, gather, local_sem.at[3]),
        pltpu.make_async_copy(spread_hbm, spread, local_sem.at[4]),
    ]
    for copy in loads:
        copy.start()

    reg = region[0]
    s = jnp.zeros(reg.shape, jnp.float32)
    for r in range(sat.shape[0]):
        s = s + jnp.where(reg == r + 1, sat[r], 0.0)
    strength[own, :] = s
    for j in range(3):
        mom[g, j, own, :] = direction[j, 0] * s

    friends = 2
    for cond in (has_up, has_dn, has_after, has_before):
        friends = friends + jnp.where(cond, 1, 0)
    pl.semaphore_wait(barrier, friends)

    def chunk_copy(p, j, way):
        where, recv = ((up_id, ag_ici), (dn_id, ag_ici), (side_id, ag_ici), (peer_id, ag_d2d))[way]
        block = mom.at[p, j, own, :]
        return pltpu.make_async_remote_copy(
            src_ref=block,
            dst_ref=block,
            send_sem=ag_send.at[way, p, j],
            recv_sem=recv.at[p, j],
            device_id=where,
            device_id_type=MESH,
        )

    def peer_arrival(p, j):
        block = mom.at[p, j, other, :]
        return pltpu.make_async_remote_copy(
            src_ref=block,
            dst_ref=block,
            send_sem=ag_send.at[3, p, j],
            recv_sem=ag_d2d.at[p, j],
            device_id=peer_id,
            device_id_type=MESH,
        )

    def when(cond, action):
        pl.when(cond)(action)

    for j in range(3):
        when(has_up, lambda: chunk_copy(g, j, 0).start())
        when(has_dn, lambda: chunk_copy(g, j, 1).start())
        chunk_copy(g, j, 2).start()

    def strength_copy(way):
        where = (peer_id, after_id, before_id)[way]
        if way == 0:
            dst = strength.at[own, :]
        else:
            dst = near_strength.at[way - 1]
        return pltpu.make_async_remote_copy(
            src_ref=strength.at[own, :],
            dst_ref=dst,
            send_sem=s_send.at[way],
            recv_sem=s_recv.at[way],
            device_id=where,
            device_id_type=MESH,
        )

    strength_copy(0).start()
    when(has_after, lambda: strength_copy(1).start())
    when(has_before, lambda: strength_copy(2).start())
    for j in range(3):
        chunk_copy(g, j, 3).start()

    for h in range(1, line + 1):
        for j in range(3):
            if h < line:

                @pl.when(o >= h)
                def _():
                    p = g - 2 * h
                    chunk_copy(p, j, 2).wait_recv()
                    when(has_up, lambda: chunk_copy(p, j, 0).start())
                    chunk_copy(p, j, 2).start()
                    chunk_copy(p, j, 3).start()

                @pl.when(o + h < line)
                def _():
                    p = g + 2 * h
                    chunk_copy(p, j, 2).wait_recv()
                    when(has_dn, lambda: chunk_copy(p, j, 1).start())
                    chunk_copy(p, j, 2).start()
                    chunk_copy(p, j, 3).start()

            def side_arrived(p):
                chunk_copy(p, j, 2).wait_recv()
                chunk_copy(p, j, 3).start()

            if h == 1:
                side_arrived(side)
            else:
                when(o >= h - 1, lambda: side_arrived(side - 2 * (h - 1)))
                when(o + h - 1 < line, lambda: side_arrived(side + 2 * (h - 1)))

    for copy in loads:
        copy.wait()
    for p in range(planes):
        for j in range(3):
            peer_arrival(p, j).wait_recv()

    step = 32
    for j in range(3):
        for top in range(0, rows_total, step):
            accs = [None] * 4
            for p in range(planes):
                m = mom[p, j, top : top + step, :]
                for q in range(4):
                    term = m * coef[g, 4 * p + q]
                    accs[q] = term if accs[q] is None else accs[q] + term
            for q in range(4):
                hi, lo = split(accs[q])
                at = (2 * j + q // 2) * rows_total + top
                lanes = slice((q % 2) * columns, (q % 2 + 1) * columns)
                zh[at : at + step, lanes] = hi
                zl[at : at + step, lanes] = lo

    nyq = [None, None]
    for b in range(6):
        band = slice(b * rows_total, (b + 1) * rows_total)
        hi, lo = zh[band, :], zl[band, :]
        res = mm(hi, tx[0, 0]) + mm(hi, tx[0, 1]) + mm(lo, tx[0, 0])
        signs = gather[b * columns : (b + 1) * columns, :]
        for q in range(2):
            lanes = slice(q * columns, (q + 1) * columns)
            band_out = slice(q * rows_total, (q + 1) * rows_total)
            cols = slice(b * columns, (b + 1) * columns)
            rhi, rlo = split(res[:, lanes])
            rh[band_out, cols] = rhi
            rl[band_out, cols] = rlo
            n = mm(hi[:, lanes], signs) + mm(lo[:, lanes], signs)
            nyq[q] = n if nyq[q] is None else nyq[q] + n
    nyq_cols = slice(6 * columns, 7 * columns)
    for q in range(2):
        band_out = slice(q * rows_total, (q + 1) * rows_total)
        rhi, rlo = split(nyq[q])
        rh[band_out, nyq_cols] = rhi
        rl[band_out, nyq_cols] = rlo

    spec = kmain.shape[2]

    def column_pass(t, b):
        cols = slice(b * columns, (b + 1) * columns)
        hi, lo = (rh, rl) if t == 0 else (gh, gl)
        hi, lo = hi[:, cols], lo[:, cols]
        return mm(ty[t, 0], hi) + mm(ty[t, 1], hi) + mm(ty[t, 0], lo)

    for k in range(2):
        spectra = [column_pass(0, 2 * j + k) for j in range(3)]
        for i in range(3):
            cols = slice((2 * i + k) * columns, (2 * i + k + 1) * columns)
            for q in range(2):
                band = slice(q * spec, (q + 1) * spec)
                total = kmain[tensor_index[i][0], k] * spectra[0][band]
                for j in (1, 2):
                    total = total + kmain[tensor_index[i][j], k] * spectra[j][band]
                hi, lo = split(total)
                gh[band, cols] = hi
                gl[band, cols] = lo
    spectrum = column_pass(0, 6)
    factors = knyq[...].reshape(12, spec)
    totals = [None, None]
    for d in range(3):
        factor = lax.dot_general(
            factors, pick[d], (((0,), (0,)), ((), ())), precision=highest, preferred_element_type=jnp.float32
        )
        moved = spectrum if d == 0 else pltpu.roll(spectrum, columns - 2 * d, 1)
        for q in range(2):
            term = factor * moved[q * spec : (q + 1) * spec]
            totals[q] = term if totals[q] is None else totals[q] + term
    for q in range(2):
        hi, lo = split(totals[q])
        gh[q * spec : (q + 1) * spec, nyq_cols] = hi
        gl[q * spec : (q + 1) * spec, nyq_cols] = lo

    back = column_pass(1, 6)
    nyq_back = [split(back[:rows_total]), split(back[rows_total:])]

    def a_copy(j):
        return pltpu.make_async_remote_copy(
            src_ref=afull.at[j, :, other, :],
            dst_ref=apeer.at[j],
            send_sem=a_send.at[j],
            recv_sem=a_recv.at[j],
            device_id=peer_id,
            device_id_type=MESH,
        )

    for j in range(3):
        for k in range(2):
            b = 2 * j + k
            back = column_pass(1, b)
            parts = [split(back[:rows_total]), split(back[rows_total:])]
            hi = jnp.concatenate([parts[0][0], parts[1][0]], axis=1)
            lo = jnp.concatenate([parts[0][1], parts[1][1]], axis=1)
            res = mm(hi, tx[1, 0]) + mm(hi, tx[1, 1]) + mm(lo, tx[1, 0])
            signs = spread[:, b * columns : (b + 1) * columns]
            for q in range(2):
                extra = mm(nyq_back[q][0], signs) + mm(nyq_back[q][1], signs)
                afull[j, 2 * k + q] = res[:, q * columns : (q + 1) * columns] + extra
        a_copy(j).start()

    def contribution(p, j):
        total = None
        for q in range(4):
            term = apeer[j, q] * coef[g, 4 * p + q]
            total = term if total is None else total + term
        return total

    def rs_copy(d, j, way):
        src, dst, ssem, rsem, where = (
            (xsend, xrecv, x_ssem, x_rsem, side_id),
            (upsend, uprecv, up_ssem, up_rsem, up_id),
            (dnsend, dnrecv, dn_ssem, dn_rsem, dn_id),
        )[way]
        return pltpu.make_async_remote_copy(
            src_ref=src.at[d, j],
            dst_ref=dst.at[d, j],
            send_sem=ssem.at[d, j],
            recv_sem=rsem.at[d, j],
            device_id=where,
            device_id_type=MESH,
        )

    def side_send(d, j):
        xsend[d, j] = contribution(2 * d + 1 - xi, j)
        rs_copy(d, j, 0).start()

    for j in range(3):
        a_copy(j).wait_recv()
        for q in range(4):
            apeer[j, q] = apeer[j, q] + afull[j, q, own, :]
        when(o + line - 1 < line, lambda: side_send(o + line - 1, j))
        when(o - line + 1 >= 0, lambda: side_send(o - line + 1, j))
    for h in range(line - 2, -1, -1):
        for j in range(3):
            if h == 0:
                side_send(o, j)
            else:
                when(o + h < line, lambda: side_send(o + h, j))
                when(o - h >= 0, lambda: side_send(o - h, j))

    strength_copy(0).wait_recv()
    for way, cond in ((1, has_before), (2, has_after)):

        @pl.when(cond)
        def _(way=way):
            strength_copy(way).wait_recv()

        @pl.when(jnp.logical_not(cond))
        def _(way=way):
            near_strength[way - 1] = jnp.zeros(near_strength.shape[1:], jnp.float32)

    full = strength[...]
    inverse = jnp.where(full > 0, 1.0 / jnp.where(full > 0, full, 1.0), 0.0)
    present = jnp.where(full > 0, 1.0, 0.0)
    row_id = lax.broadcasted_iota(jnp.int32, full.shape, 0)
    col_id = lax.broadcasted_iota(jnp.int32, full.shape, 1)

    def plane_near(v):
        total = jnp.where(row_id > 0, pltpu.roll(v, 1, 0), 0.0)
        total = total + jnp.where(row_id < rows_total - 1, pltpu.roll(v, rows_total - 1, 0), 0.0)
        total = total + jnp.where(col_id > 0, pltpu.roll(v, 1, 1), 0.0)
        return total + jnp.where(col_id < columns - 1, pltpu.roll(v, columns - 1, 1), 0.0)

    for j in range(3):
        exch[j] = plane_near(mom[g, j] * inverse)
    exch[3] = plane_near(present)
    adjacent = []
    for way in range(2):
        near_s = near_strength[way]
        there = near_s > 0
        adjacent.append(
            (jnp.where(there, 1.0 / jnp.where(there, near_s, 1.0), 0.0), jnp.where(there, 1.0, 0.0))
        )
    count = exch[3, own, :] + adjacent[0][1] + adjacent[1][1]
    mask = jnp.where(region[0] > 0, exchange_stiffness, 0.0)
    lower = jnp.maximum(g - 1, 0)
    upper = jnp.minimum(g + 1, planes - 1)
    for j in range(3):
        near = exch[j, own, :] + mom[lower, j, own, :] * adjacent[0][0]
        near = near + mom[upper, j, own, :] * adjacent[1][0]
        out[j, 0] = mask * (near - count * direction[j, 0])

    for h in range(line - 1, 0, -1):
        for j in range(3):

            def hop(d, way, cond):
                stage, arrived = ((upsend, uprecv), (dnsend, dnrecv))[way - 1]
                rs_copy(d, j, 0).wait_recv()
                stage[d, j] = contribution(2 * d + xi, j) + xrecv[d, j]

                @pl.when(cond)
                def _():
                    rs_copy(d, j, way).wait_recv()
                    stage[d, j] = stage[d, j] + arrived[d, j]

                rs_copy(d, j, way).start()

            when(o + h < line, lambda: hop(o + h, 1, has_dn))
            when(o - h >= 0, lambda: hop(o - h, 2, has_up))

    scale = 1.0 / (4 * rows_total * columns * 2 * planes)
    for j in range(3):
        rs_copy(o, j, 0).wait_recv()
        exch[j, :rows, :] = contribution(g, j) + xrecv[o, j]

        @pl.when(has_dn)
        def _():
            rs_copy(o, j, 1).wait_recv()
            exch[j, :rows, :] = exch[j, :rows, :] + uprecv[o, j]

        @pl.when(has_up)
        def _():
            rs_copy(o, j, 2).wait_recv()
            exch[j, :rows, :] = exch[j, :rows, :] + dnrecv[o, j]

        out[j, 0] = out[j, 0] + exch[j, :rows, :] * scale

    strength_copy(0).wait_send()
    when(has_after, lambda: strength_copy(1).wait_send())
    when(has_before, lambda: strength_copy(2).wait_send())
    for j in range(3):
        a_copy(j).wait_send()
        for p in range(planes):
            chunk_copy(p, j, 3).wait_send()
        for d in range(line):
            chunk_copy(2 * d + xi, j, 2).wait_send()
            rs_copy(d, j, 0).wait_send()

            @pl.when(jnp.logical_and(has_up, o >= d))
            def _():
                chunk_copy(2 * d + xi, j, 0).wait_send()

            @pl.when(jnp.logical_and(has_dn, o <= d))
            def _():
                chunk_copy(2 * d + xi, j, 1).wait_send()

            when(o < d, lambda: rs_copy(d, j, 1).wait_send())
            when(o > d, lambda: rs_copy(d, j, 2).wait_send())


def fused_local(direction, region, saturation, kernel_main, kernel_nyq):
    rows, columns = direction.shape[2:]
    planes = lax.axis_size("gz")
    groups_y = lax.axis_size("gy")
    rows_total = rows * groups_y
    spec = kernel_main.shape[2]
    line = planes // 2
    tx, ty, gather, spread, pick, coef = (
        jnp.asarray(t) for t in tables(columns, rows_total, groups_y, planes)
    )
    f32, bf16 = jnp.float32, jnp.bfloat16
    vmem = pl.BlockSpec(memory_space=pltpu.VMEM)
    smem = pl.BlockSpec(memory_space=pltpu.SMEM)
    hbm = pl.BlockSpec(memory_space=pl.ANY)
    dma = pltpu.SemaphoreType.DMA
    stage = pltpu.VMEM((line, 3, rows, columns), f32)
    return pl.pallas_call(
        fused,
        out_shape=jax.ShapeDtypeStruct(direction.shape, f32),
        in_specs=[smem, smem, vmem, vmem, vmem, vmem, hbm, hbm, hbm, hbm, hbm],
        out_specs=vmem,
        scratch_shapes=[
            pltpu.VMEM((planes, 3, rows_total, columns), f32),
            pltpu.VMEM((rows_total, columns), f32),
            pltpu.VMEM((2, rows, columns), f32),
            pltpu.VMEM((4, rows_total, columns), f32),
            pltpu.VMEM(kernel_main.shape, f32),
            pltpu.VMEM(tx.shape, bf16),
            pltpu.VMEM(ty.shape[1:], bf16),
            pltpu.VMEM(gather.shape, bf16),
            pltpu.VMEM(spread.shape, bf16),
            pltpu.VMEM((6 * rows_total, 2 * columns), bf16),
            pltpu.VMEM((6 * rows_total, 2 * columns), bf16),
            pltpu.VMEM((2 * rows_total, 7 * columns), bf16),
            pltpu.VMEM((2 * rows_total, 7 * columns), bf16),
            pltpu.VMEM((2 * spec, 7 * columns), bf16),
            pltpu.VMEM((2 * spec, 7 * columns), bf16),
            pltpu.VMEM((3, 4, rows_total, columns), f32),
            pltpu.VMEM((3, 4, rows, columns), f32),
            stage,
            stage,
            stage,
            stage,
            stage,
            stage,
            dma((5,)),
            dma((4, planes, 3)),
            dma((planes, 3)),
            dma((planes, 3)),
            dma((3,)),
            dma((3,)),
            dma((3,)),
            dma((3,)),
            dma((line, 3)),
            dma((line, 3)),
            dma((line, 3)),
            dma((line, 3)),
            dma((line, 3)),
            dma((line, 3)),
        ],
        compiler_params=pltpu.CompilerParams(
            collective_id=0, has_side_effects=True, vmem_limit_bytes=40 * 1024 * 1024
        ),
        name="field_kernel",
    )(coef, saturation, direction, region, pick, kernel_nyq, kernel_main, tx, ty, gather, spread)


def solution(mesh):
    placed = (
        P(None, ("parts", "gz"), "gy", None),
        P(("parts", "gz"), "gy", None),
        P(),
        P(None, "gz", "gy", None),
        P(None, "gz", "gy"),
    )
    small = mesh.shape["gz"] <= most_unrolled_planes and mesh.shape["gy"] == 2
    return jax.shard_map(
        fused_local if small else local,
        mesh=mesh,
        in_specs=placed,
        out_specs=P(None, ("parts", "gz"), "gy", None),
        check_vma=False,
    )
```

```python
import functools
import math

import jax
import jax.numpy as jnp
import numpy as np
from jax import lax
from jax.experimental import pallas as pl
from jax.experimental.pallas import tpu as pltpu
from jax.sharding import PartitionSpec as P

exchange_stiffness = 0.25
tensor_index = ((0, 3, 4), (3, 1, 5), (4, 5, 2))
highest = lax.Precision.HIGHEST


def with_halo(cells, sides, width):
    for axis, dim in sides:
        count = lax.axis_size(axis)
        ends = count - 1
        head = lax.slice_in_dim(cells, 0, width, axis=dim)
        tail = lax.slice_in_dim(cells, cells.shape[dim] - width, cells.shape[dim], axis=dim)
        cells = jnp.concatenate(
            [
                lax.ppermute(tail, axis, [(i, (i + 1) % count) for i in range(ends)]),
                cells,
                lax.ppermute(head, axis, [((i + 1) % count, i) for i in range(ends)]),
            ],
            axis=dim,
        )
    return cells


def phase(first, second, period):
    product = first[:, None] * second[None, :] % period
    angle = 2.0 * math.pi / period * product.astype(jnp.float32)
    return (jnp.cos(angle), jnp.sin(angle))


def slot_frequency(slot_index, bit_count):
    device = slot_index // 2
    reversed_bits = jnp.zeros_like(device)
    for b in range(bit_count):
        reversed_bits = reversed_bits + device // 2**b % 2 * 2 ** (bit_count - 1 - b)
    return 2 * reversed_bits + slot_index % 2


def row_transform(plane):
    columns = plane.shape[2]
    row_count = plane.shape[1]
    positions = jnp.arange(columns, dtype=jnp.int32)
    cosine, sine = phase(positions, positions, 2 * columns)
    table = jnp.concatenate([cosine, -sine], axis=1)
    flat = plane.reshape(3 * row_count, columns)
    both = jnp.dot(flat, table, precision=highest).reshape(3, row_count, 2, columns)
    signs = 1.0 - 2.0 * (positions % 2).astype(jnp.float32)
    nyquist = jnp.dot(flat, signs, precision=highest).reshape(3, row_count)
    return (both[:, :, 0], both[:, :, 1], nyquist)


def column_transform(real_rows, imag_rows, nyquist, cosine, sine):
    new_real = jnp.einsum("kr,crx->ckx", cosine, real_rows, precision=highest) + jnp.einsum(
        "kr,crx->ckx", sine, imag_rows, precision=highest
    )
    new_imag = jnp.einsum("kr,crx->ckx", cosine, imag_rows, precision=highest) - jnp.einsum(
        "kr,crx->ckx", sine, real_rows, precision=highest
    )
    nyq_real = jnp.einsum("kr,cr->ck", cosine, nyquist, precision=highest)
    nyq_imag = -jnp.einsum("kr,cr->ck", sine, nyquist, precision=highest)
    return (jnp.stack([new_real, new_imag], axis=1), jnp.stack([nyq_real, nyq_imag], axis=1))


def plane_transform(values, cosine, sine, direction_sign):
    real_part = values[:, 0]
    imag_part = values[:, 1]
    new_real = jnp.einsum(
        "pz,cz...->cp...", cosine, real_part, precision=highest
    ) - direction_sign * jnp.einsum("pz,cz...->cp...", sine, imag_part, precision=highest)
    new_imag = jnp.einsum(
        "pz,cz...->cp...", cosine, imag_part, precision=highest
    ) + direction_sign * jnp.einsum("pz,cz...->cp...", sine, real_part, precision=highest)
    return jnp.stack([new_real, new_imag], axis=1)


def apply_kernel(spectra, kernel):
    pieces = []
    for i in range(3):
        summed = kernel[tensor_index[i][0]] * spectra[0]
        for j in (1, 2):
            summed = summed + kernel[tensor_index[i][j]] * spectra[j]
        pieces.append(summed)
    return jnp.stack(pieces)


def local(direction, region, saturation, kernel_main, kernel_nyq):
    columns = direction.shape[3]
    own_rows = direction.shape[2]
    groups_y = lax.axis_size("gy")
    groups_z = lax.axis_size("gz")
    bit_count = groups_z.bit_length() - 1
    rows_total = own_rows * groups_y
    period_y = 2 * rows_total
    period_z = 2 * groups_z
    period_x = 2 * columns
    spec_rows = period_y // groups_y
    y_index = lax.axis_index("gy")
    magnetic = (region > 0).astype(jnp.float32)
    strength = jnp.zeros(region.shape, jnp.float32)
    for r in range(saturation.shape[0]):
        strength = strength + jnp.where(region == r + 1, saturation[r], 0.0)
    magnet_plane = (direction * strength[None])[:, 0]
    gathered = lax.all_gather(magnet_plane, "gy", axis=1, tiled=True)
    frequency = y_index * spec_rows + jnp.arange(spec_rows, dtype=jnp.int32)
    cosine, sine = phase(frequency, jnp.arange(rows_total, dtype=jnp.int32), period_y)
    real_rows, imag_rows, nyquist = row_transform(gathered)
    spec_main, spec_nyq = column_transform(real_rows, imag_rows, nyquist, cosine, sine)
    slot_freq = slot_frequency(jnp.arange(period_z, dtype=jnp.int32), bit_count)
    plane_ids = jnp.arange(groups_z, dtype=jnp.int32)
    sent_main, sent_nyq = (
        lax.all_to_all(spec_main[:, :, None], "gz", split_axis=3, concat_axis=2, tiled=True),
        lax.all_to_all(spec_nyq[:, :, None], "gz", split_axis=3, concat_axis=2, tiled=True),
    )
    cosine, sine = phase(slot_freq, plane_ids, period_z)
    done_main = plane_transform(sent_main, cosine, sine, -1.0)
    done_nyq = plane_transform(sent_nyq, cosine, sine, -1.0)
    full_main, full_nyq = (
        lax.all_to_all(done_main, "gz", split_axis=2, concat_axis=3, tiled=True),
        lax.all_to_all(done_nyq, "gz", split_axis=2, concat_axis=3, tiled=True),
    )
    field_main = apply_kernel(full_main, kernel_main)
    field_nyq = apply_kernel(full_nyq, kernel_nyq)
    out_main, out_nyq = (
        lax.all_to_all(field_main, "gz", split_axis=3, concat_axis=2, tiled=True),
        lax.all_to_all(field_nyq, "gz", split_axis=3, concat_axis=2, tiled=True),
    )
    cosine, sine = phase(plane_ids, slot_freq, period_z)
    back_main = plane_transform(out_main, cosine, sine, 1.0)
    back_nyq = plane_transform(out_nyq, cosine, sine, 1.0)
    plane_main, plane_nyq = (
        lax.all_to_all(back_main, "gz", split_axis=2, concat_axis=3, tiled=True),
        lax.all_to_all(back_nyq, "gz", split_axis=2, concat_axis=3, tiled=True),
    )
    plane_main = plane_main[:, :, 0]
    plane_nyq = plane_nyq[:, :, 0]
    frequency = y_index * spec_rows + jnp.arange(spec_rows, dtype=jnp.int32)
    cosine, sine = phase(jnp.arange(rows_total, dtype=jnp.int32), frequency, period_y)
    term_real = jnp.einsum("yk,ckx->cyx", cosine, plane_main[:, 0], precision=highest) - jnp.einsum(
        "yk,ckx->cyx", sine, plane_main[:, 1], precision=highest
    )
    term_imag = jnp.einsum("yk,ckx->cyx", cosine, plane_main[:, 1], precision=highest) + jnp.einsum(
        "yk,ckx->cyx", sine, plane_main[:, 0], precision=highest
    )
    nyq_real = jnp.einsum("yk,ck->cy", cosine, plane_nyq[:, 0], precision=highest) - jnp.einsum(
        "yk,ck->cy", sine, plane_nyq[:, 1], precision=highest
    )
    nyq_imag = jnp.einsum("yk,ck->cy", cosine, plane_nyq[:, 1], precision=highest) + jnp.einsum(
        "yk,ck->cy", sine, plane_nyq[:, 0], precision=highest
    )
    rows_main, rows_nyq = (
        lax.psum_scatter(
            jnp.stack([term_real, term_imag], axis=1), "gy", scatter_dimension=2, tiled=True
        ),
        lax.psum_scatter(
            jnp.stack([nyq_real, nyq_imag], axis=1), "gy", scatter_dimension=2, tiled=True
        ),
    )
    positions = jnp.arange(columns, dtype=jnp.int32)
    cosine, sine = phase(positions, positions, period_x)
    weights = jnp.where(positions == 0, 1.0, 2.0).astype(jnp.float32)[:, None]
    table = jnp.concatenate([weights * cosine, -weights * sine], axis=0)
    flat = jnp.concatenate([rows_main[:, 0], rows_main[:, 1]], axis=2).reshape(
        3 * own_rows, 2 * columns
    )
    signs = 1.0 - 2.0 * (positions % 2).astype(jnp.float32)
    demag = jnp.dot(flat, table, precision=highest).reshape(3, own_rows, columns)
    demag = demag + rows_nyq[:, 0][:, :, None] * signs[None, None, :]
    demag = demag * (1.0 / (period_x * period_y * period_z))
    moment = direction * magnetic[None]
    stacked = jnp.concatenate([moment, magnetic[None]], axis=0)
    rim = with_halo(stacked, (("gz", 1), ("gy", 2)), 1)
    centre = rim[:, 1:2, 1:-1]
    near = rim[:, 0:1, 1:-1] + rim[:, 2:3, 1:-1] + rim[:, 1:2, :-2] + rim[:, 1:2, 2:]
    padded_x = jnp.pad(centre, ((0, 0), (0, 0), (0, 0), (1, 1)))
    near = near + padded_x[..., :-2] + padded_x[..., 2:]
    exchange = exchange_stiffness * magnetic[None] * (near[:3] - near[3:4] * direction)
    return demag[:, None] + exchange


MESH = pl.DeviceIdType.MESH
most_unrolled_planes = 16


def halves(table):
    high = table.astype(np.float32).astype(jnp.bfloat16)
    low = (table - high.astype(np.float64)).astype(np.float32).astype(jnp.bfloat16)
    return np.stack([high, low])


@functools.lru_cache(maxsize=None)
def tables(columns, rows_total, groups_y, groups_z):
    x = np.arange(columns)
    ang = np.pi / columns * (np.outer(x, x) % (2 * columns))
    c, s = np.cos(ang), np.sin(ang)
    fwd = np.block([[c, -s], [s, c]])
    w = np.where(x == 0, 1.0, 2.0)[:, None]
    inv = np.block([[w * c, w * s], [-w * s, w * c]])
    tx = np.stack([halves(fwd), halves(inv)])
    spec = 2 * rows_total // groups_y
    y = np.arange(rows_total)
    ty = []
    for g in range(groups_y):
        ky = g * spec + np.arange(spec)
        ang = np.pi / rows_total * (np.outer(ky, y) % (2 * rows_total))
        c, s = np.cos(ang), np.sin(ang)
        f = np.block([[c, s], [-s, c]])
        ty.append(np.stack([halves(f), halves(f.T)]))
    ty = np.stack(ty)
    signs = 1.0 - 2.0 * (x % 2)
    gather = np.zeros((6 * columns, columns))
    spread = np.zeros((columns, 6 * columns))
    for b in range(6):
        gather[b * columns : (b + 1) * columns, b] = signs
        gather[b * columns : (b + 1) * columns, b + 6] = signs
        spread[b, b * columns : (b + 1) * columns] = signs
    pick = np.zeros((3, 12, columns))
    for d in range(3):
        for i in range(3):
            for k in range(2):
                pick[d, tensor_index[i][(i + d) % 3] * 2 + k, i * 2 + k] = 1.0
    bits = groups_z.bit_length() - 1
    coef = np.zeros((groups_z, 4 * groups_z))
    plane = np.arange(groups_z)
    for g in range(groups_z):
        rev = sum(((g >> b) & 1) << (bits - 1 - b) for b in range(bits))
        for k in range(2):
            ang = np.pi / groups_z * ((2 * rev + k) * plane % (2 * groups_z))
            coef[g, 2 * k :: 4] = np.cos(ang)
            coef[g, 2 * k + 1 :: 4] = -np.sin(ang)
    return (
        tx,
        ty,
        gather.astype(jnp.bfloat16),
        spread.astype(jnp.bfloat16),
        pick.astype(np.float32),
        coef.astype(np.float32),
    )


def split(value):
    high = value.astype(jnp.bfloat16)
    return high, (value - high.astype(jnp.float32)).astype(jnp.bfloat16)


def mm(a, b):
    return jnp.dot(a, b, preferred_element_type=jnp.float32)


def fused(
    coef,
    sat,
    direction_hbm,
    region_hbm,
    pick_hbm,
    knyq_hbm,
    kmain_hbm,
    tx_hbm,
    ty_hbm,
    gather_hbm,
    spread_hbm,
    out,
    direction,
    region,
    pick,
    knyq,
    mom,
    strength,
    near_strength,
    exch,
    kmain,
    tx,
    ty,
    gather,
    spread,
    zh,
    zl,
    rh,
    rl,
    gh,
    gl,
    afull,
    apeer,
    xsend,
    xrecv,
    upsend,
    uprecv,
    dnsend,
    dnrecv,
    local_sem,
    ag_send,
    ag_ici,
    ag_d2d,
    s_send,
    s_recv,
    a_send,
    a_recv,
    x_ssem,
    x_rsem,
    up_ssem,
    up_rsem,
    dn_ssem,
    dn_rsem,
):
    planes = mom.shape[0]
    line = planes // 2
    rows_total = mom.shape[2]
    columns = mom.shape[3]
    rows = direction.shape[2]
    g = lax.axis_index("gz")
    c = lax.axis_index("gy")
    o = g // 2
    xi = g % 2
    side = g + 1 - 2 * xi
    own = pl.ds(pl.multiple_of(c * rows, rows), rows)
    other = pl.ds(pl.multiple_of((1 - c) * rows, rows), rows)
    peer_id = {"gz": g, "gy": 1 - c}
    side_id = {"gz": side, "gy": c}
    up_id = {"gz": g + 2, "gy": c}
    dn_id = {"gz": g - 2, "gy": c}
    after_id = {"gz": g + 1, "gy": c}
    before_id = {"gz": g - 1, "gy": c}
    has_up = o < line - 1
    has_dn = o > 0
    has_after = g < planes - 1
    has_before = g > 0

    barrier = pltpu.get_barrier_semaphore()
    pl.semaphore_signal(barrier, inc=1, device_id=peer_id, device_id_type=MESH)
    pl.semaphore_signal(barrier, inc=1, device_id=side_id, device_id_type=MESH)
    for cond, where in ((has_up, up_id), (has_dn, dn_id), (has_after, after_id), (has_before, before_id)):

        @pl.when(cond)
        def _(where=where):
            pl.semaphore_signal(barrier, inc=1, device_id=where, device_id_type=MESH)

    first = [
        pltpu.make_async_copy(direction_hbm, direction, local_sem.at[5]),
        pltpu.make_async_copy(region_hbm, region, local_sem.at[6]),
    ]
    for copy in first:
        copy.start()
    loads = [
        pltpu.make_async_copy(kmain_hbm, kmain, local_sem.at[0]),
        pltpu.make_async_copy(tx_hbm, tx, local_sem.at[1]),
        pltpu.make_async_copy(ty_hbm.at[c], ty, local_sem.at[2]),
        pltpu.make_async_copy(gather_hbm, gather, local_sem.at[3]),
        pltpu.make_async_copy(spread_hbm, spread, local_sem.at[4]),
        pltpu.make_async_copy(pick_hbm, pick, local_sem.at[7]),
        pltpu.make_async_copy(knyq_hbm, knyq, local_sem.at[8]),
    ]
    for copy in first:
        copy.wait()
    for copy in loads:
        copy.start()

    reg = region[0]
    s = jnp.zeros(reg.shape, jnp.float32)
    for r in range(sat.shape[0]):
        s = s + jnp.where(reg == r + 1, sat[r], 0.0)
    strength[own, :] = s
    for j in range(3):
        mom[g, j, own, :] = direction[j, 0] * s

    friends = 2
    for cond in (has_up, has_dn, has_after, has_before):
        friends = friends + jnp.where(cond, 1, 0)
    pl.semaphore_wait(barrier, friends)

    def chunk_copy(p, j, way):
        where, recv = ((up_id, ag_ici), (dn_id, ag_ici), (side_id, ag_ici), (peer_id, ag_d2d))[way]
        block = mom.at[p, j, own, :]
        return pltpu.make_async_remote_copy(
            src_ref=block,
            dst_ref=block,
            send_sem=ag_send.at[way, p, j],
            recv_sem=recv.at[p, j],
            device_id=where,
            device_id_type=MESH,
        )

    def peer_arrival(p, j):
        block = mom.at[p, j, other, :]
        return pltpu.make_async_remote_copy(
            src_ref=block,
            dst_ref=block,
            send_sem=ag_send.at[3, p, j],
            recv_sem=ag_d2d.at[p, j],
            device_id=peer_id,
            device_id_type=MESH,
        )

    def when(cond, action):
        pl.when(cond)(action)

    for j in range(3):
        when(has_up, lambda: chunk_copy(g, j, 0).start())
        when(has_dn, lambda: chunk_copy(g, j, 1).start())
        chunk_copy(g, j, 2).start()

    def strength_copy(way):
        where = (peer_id, after_id, before_id)[way]
        if way == 0:
            dst = strength.at[own, :]
        else:
            dst = near_strength.at[way - 1]
        return pltpu.make_async_remote_copy(
            src_ref=strength.at[own, :],
            dst_ref=dst,
            send_sem=s_send.at[way],
            recv_sem=s_recv.at[way],
            device_id=where,
            device_id_type=MESH,
        )

    strength_copy(0).start()
    when(has_after, lambda: strength_copy(1).start())
    when(has_before, lambda: strength_copy(2).start())
    for j in range(3):
        chunk_copy(g, j, 3).start()

    for h in range(1, line + 1):
        for j in range(3):
            if h < line:

                @pl.when(o >= h)
                def _():
                    p = g - 2 * h
                    chunk_copy(p, j, 2).wait_recv()
                    when(has_up, lambda: chunk_copy(p, j, 0).start())
                    chunk_copy(p, j, 2).start()
                    chunk_copy(p, j, 3).start()

                @pl.when(o + h < line)
                def _():
                    p = g + 2 * h
                    chunk_copy(p, j, 2).wait_recv()
                    when(has_dn, lambda: chunk_copy(p, j, 1).start())
                    chunk_copy(p, j, 2).start()
                    chunk_copy(p, j, 3).start()

            def side_arrived(p):
                chunk_copy(p, j, 2).wait_recv()
                chunk_copy(p, j, 3).start()

            if h == 1:
                side_arrived(side)
            else:
                when(o >= h - 1, lambda: side_arrived(side - 2 * (h - 1)))
                when(o + h - 1 < line, lambda: side_arrived(side + 2 * (h - 1)))

    for copy in loads:
        copy.wait()
    for p in range(planes):
        for j in range(3):
            peer_arrival(p, j).wait_recv()

    step = 32
    for j in range(3):
        for top in range(0, rows_total, step):
            accs = [None] * 4
            for p in range(planes):
                m = mom[p, j, top : top + step, :]
                for q in range(4):
                    term = m * coef[g, 4 * p + q]
                    accs[q] = term if accs[q] is None else accs[q] + term
            for q in range(4):
                hi, lo = split(accs[q])
                at = (2 * j + q // 2) * rows_total + top
                lanes = slice((q % 2) * columns, (q % 2 + 1) * columns)
                zh[at : at + step, lanes] = hi
                zl[at : at + step, lanes] = lo

    nyq = [None, None]
    for b in range(6):
        band = slice(b * rows_total, (b + 1) * rows_total)
        hi, lo = zh[band, :], zl[band, :]
        res = mm(hi, tx[0, 0]) + mm(hi, tx[0, 1]) + mm(lo, tx[0, 0])
        signs = gather[b * columns : (b + 1) * columns, :]
        for q in range(2):
            lanes = slice(q * columns, (q + 1) * columns)
            band_out = slice(q * rows_total, (q + 1) * rows_total)
            cols = slice(b * columns, (b + 1) * columns)
            rhi, rlo = split(res[:, lanes])
            rh[band_out, cols] = rhi
            rl[band_out, cols] = rlo
            n = mm(hi[:, lanes], signs) + mm(lo[:, lanes], signs)
            nyq[q] = n if nyq[q] is None else nyq[q] + n
    nyq_cols = slice(6 * columns, 7 * columns)
    for q in range(2):
        band_out = slice(q * rows_total, (q + 1) * rows_total)
        rhi, rlo = split(nyq[q])
        rh[band_out, nyq_cols] = rhi
        rl[band_out, nyq_cols] = rlo

    spec = kmain.shape[2]

    def column_pass(t, b):
        cols = slice(b * columns, (b + 1) * columns)
        hi, lo = (rh, rl) if t == 0 else (gh, gl)
        hi, lo = hi[:, cols], lo[:, cols]
        return mm(ty[t, 0], hi) + mm(ty[t, 1], hi) + mm(ty[t, 0], lo)

    for k in range(2):
        spectra = [column_pass(0, 2 * j + k) for j in range(3)]
        for i in range(3):
            cols = slice((2 * i + k) * columns, (2 * i + k + 1) * columns)
            for q in range(2):
                band = slice(q * spec, (q + 1) * spec)
                total = kmain[tensor_index[i][0], k] * spectra[0][band]
                for j in (1, 2):
                    total = total + kmain[tensor_index[i][j], k] * spectra[j][band]
                hi, lo = split(total)
                gh[band, cols] = hi
                gl[band, cols] = lo
    spectrum = column_pass(0, 6)
    factors = knyq[...].reshape(12, spec)
    totals = [None, None]
    for d in range(3):
        factor = lax.dot_general(
            factors, pick[d], (((0,), (0,)), ((), ())), precision=highest, preferred_element_type=jnp.float32
        )
        moved = spectrum if d == 0 else pltpu.roll(spectrum, columns - 2 * d, 1)
        for q in range(2):
            term = factor * moved[q * spec : (q + 1) * spec]
            totals[q] = term if totals[q] is None else totals[q] + term
    for q in range(2):
        hi, lo = split(totals[q])
        gh[q * spec : (q + 1) * spec, nyq_cols] = hi
        gl[q * spec : (q + 1) * spec, nyq_cols] = lo

    back = column_pass(1, 6)
    nyq_back = [split(back[:rows_total]), split(back[rows_total:])]

    def a_copy(j):
        return pltpu.make_async_remote_copy(
            src_ref=afull.at[j, :, other, :],
            dst_ref=apeer.at[j],
            send_sem=a_send.at[j],
            recv_sem=a_recv.at[j],
            device_id=peer_id,
            device_id_type=MESH,
        )

    for j in range(3):
        for k in range(2):
            b = 2 * j + k
            back = column_pass(1, b)
            parts = [split(back[:rows_total]), split(back[rows_total:])]
            hi = jnp.concatenate([parts[0][0], parts[1][0]], axis=1)
            lo = jnp.concatenate([parts[0][1], parts[1][1]], axis=1)
            res = mm(hi, tx[1, 0]) + mm(hi, tx[1, 1]) + mm(lo, tx[1, 0])
            signs = spread[:, b * columns : (b + 1) * columns]
            for q in range(2):
                extra = mm(nyq_back[q][0], signs) + mm(nyq_back[q][1], signs)
                afull[j, 2 * k + q] = res[:, q * columns : (q + 1) * columns] + extra
        a_copy(j).start()

    def contribution(p, j):
        total = None
        for q in range(4):
            term = apeer[j, q] * coef[g, 4 * p + q]
            total = term if total is None else total + term
        return total

    def rs_copy(d, j, way):
        src, dst, ssem, rsem, where = (
            (xsend, xrecv, x_ssem, x_rsem, side_id),
            (upsend, uprecv, up_ssem, up_rsem, up_id),
            (dnsend, dnrecv, dn_ssem, dn_rsem, dn_id),
        )[way]
        return pltpu.make_async_remote_copy(
            src_ref=src.at[d, j],
            dst_ref=dst.at[d, j],
            send_sem=ssem.at[d, j],
            recv_sem=rsem.at[d, j],
            device_id=where,
            device_id_type=MESH,
        )

    def side_send(d, j):
        xsend[d, j] = contribution(2 * d + 1 - xi, j)
        rs_copy(d, j, 0).start()

    for j in range(3):
        a_copy(j).wait_recv()
        for q in range(4):
            apeer[j, q] = apeer[j, q] + afull[j, q, own, :]
        when(o + line - 1 < line, lambda: side_send(o + line - 1, j))
        when(o - line + 1 >= 0, lambda: side_send(o - line + 1, j))
    for h in range(line - 2, -1, -1):
        for j in range(3):
            if h == 0:
                side_send(o, j)
            else:
                when(o + h < line, lambda: side_send(o + h, j))
                when(o - h >= 0, lambda: side_send(o - h, j))

    strength_copy(0).wait_recv()
    for way, cond in ((1, has_before), (2, has_after)):

        @pl.when(cond)
        def _(way=way):
            strength_copy(way).wait_recv()

        @pl.when(jnp.logical_not(cond))
        def _(way=way):
            near_strength[way - 1] = jnp.zeros(near_strength.shape[1:], jnp.float32)

    full = strength[...]
    inverse = jnp.where(full > 0, 1.0 / jnp.where(full > 0, full, 1.0), 0.0)
    present = jnp.where(full > 0, 1.0, 0.0)
    row_id = lax.broadcasted_iota(jnp.int32, full.shape, 0)
    col_id = lax.broadcasted_iota(jnp.int32, full.shape, 1)

    def plane_near(v):
        total = jnp.where(row_id > 0, pltpu.roll(v, 1, 0), 0.0)
        total = total + jnp.where(row_id < rows_total - 1, pltpu.roll(v, rows_total - 1, 0), 0.0)
        total = total + jnp.where(col_id > 0, pltpu.roll(v, 1, 1), 0.0)
        return total + jnp.where(col_id < columns - 1, pltpu.roll(v, columns - 1, 1), 0.0)

    for j in range(3):
        exch[j] = plane_near(mom[g, j] * inverse)
    exch[3] = plane_near(present)
    adjacent = []
    for way in range(2):
        near_s = near_strength[way]
        there = near_s > 0
        adjacent.append(
            (jnp.where(there, 1.0 / jnp.where(there, near_s, 1.0), 0.0), jnp.where(there, 1.0, 0.0))
        )
    count = exch[3, own, :] + adjacent[0][1] + adjacent[1][1]
    mask = jnp.where(region[0] > 0, exchange_stiffness, 0.0)
    lower = jnp.maximum(g - 1, 0)
    upper = jnp.minimum(g + 1, planes - 1)
    for j in range(3):
        near = exch[j, own, :] + mom[lower, j, own, :] * adjacent[0][0]
        near = near + mom[upper, j, own, :] * adjacent[1][0]
        out[j, 0] = mask * (near - count * direction[j, 0])

    for h in range(line - 1, 0, -1):
        for j in range(3):

            def hop(d, way, cond):
                stage, arrived = ((upsend, uprecv), (dnsend, dnrecv))[way - 1]
                rs_copy(d, j, 0).wait_recv()
                stage[d, j] = contribution(2 * d + xi, j) + xrecv[d, j]

                @pl.when(cond)
                def _():
                    rs_copy(d, j, way).wait_recv()
                    stage[d, j] = stage[d, j] + arrived[d, j]

                rs_copy(d, j, way).start()

            when(o + h < line, lambda: hop(o + h, 1, has_dn))
            when(o - h >= 0, lambda: hop(o - h, 2, has_up))

    scale = 1.0 / (4 * rows_total * columns * 2 * planes)
    for j in range(3):
        rs_copy(o, j, 0).wait_recv()
        exch[j, :rows, :] = contribution(g, j) + xrecv[o, j]

        @pl.when(has_dn)
        def _():
            rs_copy(o, j, 1).wait_recv()
            exch[j, :rows, :] = exch[j, :rows, :] + uprecv[o, j]

        @pl.when(has_up)
        def _():
            rs_copy(o, j, 2).wait_recv()
            exch[j, :rows, :] = exch[j, :rows, :] + dnrecv[o, j]

        out[j, 0] = out[j, 0] + exch[j, :rows, :] * scale

    strength_copy(0).wait_send()
    when(has_after, lambda: strength_copy(1).wait_send())
    when(has_before, lambda: strength_copy(2).wait_send())
    for j in range(3):
        a_copy(j).wait_send()
        for p in range(planes):
            chunk_copy(p, j, 3).wait_send()
        for d in range(line):
            chunk_copy(2 * d + xi, j, 2).wait_send()
            rs_copy(d, j, 0).wait_send()

            @pl.when(jnp.logical_and(has_up, o >= d))
            def _():
                chunk_copy(2 * d + xi, j, 0).wait_send()

            @pl.when(jnp.logical_and(has_dn, o <= d))
            def _():
                chunk_copy(2 * d + xi, j, 1).wait_send()

            when(o < d, lambda: rs_copy(d, j, 1).wait_send())
            when(o > d, lambda: rs_copy(d, j, 2).wait_send())


def fused_local(direction, region, saturation, kernel_main, kernel_nyq):
    rows, columns = direction.shape[2:]
    planes = lax.axis_size("gz")
    groups_y = lax.axis_size("gy")
    rows_total = rows * groups_y
    spec = kernel_main.shape[2]
    line = planes // 2
    tx, ty, gather, spread, pick, coef = (
        jnp.asarray(t) for t in tables(columns, rows_total, groups_y, planes)
    )
    f32, bf16 = jnp.float32, jnp.bfloat16
    vmem = pl.BlockSpec(memory_space=pltpu.VMEM)
    smem = pl.BlockSpec(memory_space=pltpu.SMEM)
    hbm = pl.BlockSpec(memory_space=pltpu.HBM)
    dma = pltpu.SemaphoreType.DMA
    stage = pltpu.VMEM((line, 3, rows, columns), f32)
    return pl.pallas_call(
        fused,
        out_shape=jax.ShapeDtypeStruct(direction.shape, f32),
        in_specs=[smem, smem, hbm, hbm, hbm, hbm, hbm, hbm, hbm, hbm, hbm],
        out_specs=vmem,
        scratch_shapes=[
            pltpu.VMEM(direction.shape, f32),
            pltpu.VMEM(region.shape, jnp.int32),
            pltpu.VMEM(pick.shape, f32),
            pltpu.VMEM(kernel_nyq.shape, f32),
            pltpu.VMEM((planes, 3, rows_total, columns), f32),
            pltpu.VMEM((rows_total, columns), f32),
            pltpu.VMEM((2, rows, columns), f32),
            pltpu.VMEM((4, rows_total, columns), f32),
            pltpu.VMEM(kernel_main.shape, f32),
            pltpu.VMEM(tx.shape, bf16),
            pltpu.VMEM(ty.shape[1:], bf16),
            pltpu.VMEM(gather.shape, bf16),
            pltpu.VMEM(spread.shape, bf16),
            pltpu.VMEM((6 * rows_total, 2 * columns), bf16),
            pltpu.VMEM((6 * rows_total, 2 * columns), bf16),
            pltpu.VMEM((2 * rows_total, 7 * columns), bf16),
            pltpu.VMEM((2 * rows_total, 7 * columns), bf16),
            pltpu.VMEM((2 * spec, 7 * columns), bf16),
            pltpu.VMEM((2 * spec, 7 * columns), bf16),
            pltpu.VMEM((3, 4, rows_total, columns), f32),
            pltpu.VMEM((3, 4, rows, columns), f32),
            stage,
            stage,
            stage,
            stage,
            stage,
            stage,
            dma((9,)),
            dma((4, planes, 3)),
            dma((planes, 3)),
            dma((planes, 3)),
            dma((3,)),
            dma((3,)),
            dma((3,)),
            dma((3,)),
            dma((line, 3)),
            dma((line, 3)),
            dma((line, 3)),
            dma((line, 3)),
            dma((line, 3)),
            dma((line, 3)),
        ],
        compiler_params=pltpu.CompilerParams(
            collective_id=0, has_side_effects=True, vmem_limit_bytes=67043328
        ),
        name="field_kernel",
    )(coef, saturation, direction, region, pick, kernel_nyq, kernel_main, tx, ty, gather, spread)


def solution(mesh):
    placed = (
        P(None, ("parts", "gz"), "gy", None),
        P(("parts", "gz"), "gy", None),
        P(),
        P(None, "gz", "gy", None),
        P(None, "gz", "gy"),
    )
    small = mesh.shape["gz"] <= most_unrolled_planes and mesh.shape["gy"] == 2
    return jax.shard_map(
        fused_local if small else local,
        mesh=mesh,
        in_specs=placed,
        out_specs=P(None, ("parts", "gz"), "gy", None),
        check_vma=False,
    )
```

```python
import functools
import math

import jax
import jax.numpy as jnp
import numpy as np
from jax import lax
from jax.experimental import pallas as pl
from jax.experimental.pallas import tpu as pltpu
from jax.sharding import PartitionSpec as P

exchange_stiffness = 0.25
tensor_index = ((0, 3, 4), (3, 1, 5), (4, 5, 2))
highest = lax.Precision.HIGHEST


def with_halo(cells, sides, width):
    for axis, dim in sides:
        count = lax.axis_size(axis)
        ends = count - 1
        head = lax.slice_in_dim(cells, 0, width, axis=dim)
        tail = lax.slice_in_dim(cells, cells.shape[dim] - width, cells.shape[dim], axis=dim)
        cells = jnp.concatenate(
            [
                lax.ppermute(tail, axis, [(i, (i + 1) % count) for i in range(ends)]),
                cells,
                lax.ppermute(head, axis, [((i + 1) % count, i) for i in range(ends)]),
            ],
            axis=dim,
        )
    return cells


def phase(first, second, period):
    product = first[:, None] * second[None, :] % period
    angle = 2.0 * math.pi / period * product.astype(jnp.float32)
    return (jnp.cos(angle), jnp.sin(angle))


def slot_frequency(slot_index, bit_count):
    device = slot_index // 2
    reversed_bits = jnp.zeros_like(device)
    for b in range(bit_count):
        reversed_bits = reversed_bits + device // 2**b % 2 * 2 ** (bit_count - 1 - b)
    return 2 * reversed_bits + slot_index % 2


def row_transform(plane):
    columns = plane.shape[2]
    row_count = plane.shape[1]
    positions = jnp.arange(columns, dtype=jnp.int32)
    cosine, sine = phase(positions, positions, 2 * columns)
    table = jnp.concatenate([cosine, -sine], axis=1)
    flat = plane.reshape(3 * row_count, columns)
    both = jnp.dot(flat, table, precision=highest).reshape(3, row_count, 2, columns)
    signs = 1.0 - 2.0 * (positions % 2).astype(jnp.float32)
    nyquist = jnp.dot(flat, signs, precision=highest).reshape(3, row_count)
    return (both[:, :, 0], both[:, :, 1], nyquist)


def column_transform(real_rows, imag_rows, nyquist, cosine, sine):
    new_real = jnp.einsum("kr,crx->ckx", cosine, real_rows, precision=highest) + jnp.einsum(
        "kr,crx->ckx", sine, imag_rows, precision=highest
    )
    new_imag = jnp.einsum("kr,crx->ckx", cosine, imag_rows, precision=highest) - jnp.einsum(
        "kr,crx->ckx", sine, real_rows, precision=highest
    )
    nyq_real = jnp.einsum("kr,cr->ck", cosine, nyquist, precision=highest)
    nyq_imag = -jnp.einsum("kr,cr->ck", sine, nyquist, precision=highest)
    return (jnp.stack([new_real, new_imag], axis=1), jnp.stack([nyq_real, nyq_imag], axis=1))


def plane_transform(values, cosine, sine, direction_sign):
    real_part = values[:, 0]
    imag_part = values[:, 1]
    new_real = jnp.einsum(
        "pz,cz...->cp...", cosine, real_part, precision=highest
    ) - direction_sign * jnp.einsum("pz,cz...->cp...", sine, imag_part, precision=highest)
    new_imag = jnp.einsum(
        "pz,cz...->cp...", cosine, imag_part, precision=highest
    ) + direction_sign * jnp.einsum("pz,cz...->cp...", sine, real_part, precision=highest)
    return jnp.stack([new_real, new_imag], axis=1)


def apply_kernel(spectra, kernel):
    pieces = []
    for i in range(3):
        summed = kernel[tensor_index[i][0]] * spectra[0]
        for j in (1, 2):
            summed = summed + kernel[tensor_index[i][j]] * spectra[j]
        pieces.append(summed)
    return jnp.stack(pieces)


def local(direction, region, saturation, kernel_main, kernel_nyq):
    columns = direction.shape[3]
    own_rows = direction.shape[2]
    groups_y = lax.axis_size("gy")
    groups_z = lax.axis_size("gz")
    bit_count = groups_z.bit_length() - 1
    rows_total = own_rows * groups_y
    period_y = 2 * rows_total
    period_z = 2 * groups_z
    period_x = 2 * columns
    spec_rows = period_y // groups_y
    y_index = lax.axis_index("gy")
    magnetic = (region > 0).astype(jnp.float32)
    strength = jnp.zeros(region.shape, jnp.float32)
    for r in range(saturation.shape[0]):
        strength = strength + jnp.where(region == r + 1, saturation[r], 0.0)
    magnet_plane = (direction * strength[None])[:, 0]
    gathered = lax.all_gather(magnet_plane, "gy", axis=1, tiled=True)
    frequency = y_index * spec_rows + jnp.arange(spec_rows, dtype=jnp.int32)
    cosine, sine = phase(frequency, jnp.arange(rows_total, dtype=jnp.int32), period_y)
    real_rows, imag_rows, nyquist = row_transform(gathered)
    spec_main, spec_nyq = column_transform(real_rows, imag_rows, nyquist, cosine, sine)
    slot_freq = slot_frequency(jnp.arange(period_z, dtype=jnp.int32), bit_count)
    plane_ids = jnp.arange(groups_z, dtype=jnp.int32)
    sent_main, sent_nyq = (
        lax.all_to_all(spec_main[:, :, None], "gz", split_axis=3, concat_axis=2, tiled=True),
        lax.all_to_all(spec_nyq[:, :, None], "gz", split_axis=3, concat_axis=2, tiled=True),
    )
    cosine, sine = phase(slot_freq, plane_ids, period_z)
    done_main = plane_transform(sent_main, cosine, sine, -1.0)
    done_nyq = plane_transform(sent_nyq, cosine, sine, -1.0)
    full_main, full_nyq = (
        lax.all_to_all(done_main, "gz", split_axis=2, concat_axis=3, tiled=True),
        lax.all_to_all(done_nyq, "gz", split_axis=2, concat_axis=3, tiled=True),
    )
    field_main = apply_kernel(full_main, kernel_main)
    field_nyq = apply_kernel(full_nyq, kernel_nyq)
    out_main, out_nyq = (
        lax.all_to_all(field_main, "gz", split_axis=3, concat_axis=2, tiled=True),
        lax.all_to_all(field_nyq, "gz", split_axis=3, concat_axis=2, tiled=True),
    )
    cosine, sine = phase(plane_ids, slot_freq, period_z)
    back_main = plane_transform(out_main, cosine, sine, 1.0)
    back_nyq = plane_transform(out_nyq, cosine, sine, 1.0)
    plane_main, plane_nyq = (
        lax.all_to_all(back_main, "gz", split_axis=2, concat_axis=3, tiled=True),
        lax.all_to_all(back_nyq, "gz", split_axis=2, concat_axis=3, tiled=True),
    )
    plane_main = plane_main[:, :, 0]
    plane_nyq = plane_nyq[:, :, 0]
    frequency = y_index * spec_rows + jnp.arange(spec_rows, dtype=jnp.int32)
    cosine, sine = phase(jnp.arange(rows_total, dtype=jnp.int32), frequency, period_y)
    term_real = jnp.einsum("yk,ckx->cyx", cosine, plane_main[:, 0], precision=highest) - jnp.einsum(
        "yk,ckx->cyx", sine, plane_main[:, 1], precision=highest
    )
    term_imag = jnp.einsum("yk,ckx->cyx", cosine, plane_main[:, 1], precision=highest) + jnp.einsum(
        "yk,ckx->cyx", sine, plane_main[:, 0], precision=highest
    )
    nyq_real = jnp.einsum("yk,ck->cy", cosine, plane_nyq[:, 0], precision=highest) - jnp.einsum(
        "yk,ck->cy", sine, plane_nyq[:, 1], precision=highest
    )
    nyq_imag = jnp.einsum("yk,ck->cy", cosine, plane_nyq[:, 1], precision=highest) + jnp.einsum(
        "yk,ck->cy", sine, plane_nyq[:, 0], precision=highest
    )
    rows_main, rows_nyq = (
        lax.psum_scatter(
            jnp.stack([term_real, term_imag], axis=1), "gy", scatter_dimension=2, tiled=True
        ),
        lax.psum_scatter(
            jnp.stack([nyq_real, nyq_imag], axis=1), "gy", scatter_dimension=2, tiled=True
        ),
    )
    positions = jnp.arange(columns, dtype=jnp.int32)
    cosine, sine = phase(positions, positions, period_x)
    weights = jnp.where(positions == 0, 1.0, 2.0).astype(jnp.float32)[:, None]
    table = jnp.concatenate([weights * cosine, -weights * sine], axis=0)
    flat = jnp.concatenate([rows_main[:, 0], rows_main[:, 1]], axis=2).reshape(
        3 * own_rows, 2 * columns
    )
    signs = 1.0 - 2.0 * (positions % 2).astype(jnp.float32)
    demag = jnp.dot(flat, table, precision=highest).reshape(3, own_rows, columns)
    demag = demag + rows_nyq[:, 0][:, :, None] * signs[None, None, :]
    demag = demag * (1.0 / (period_x * period_y * period_z))
    moment = direction * magnetic[None]
    stacked = jnp.concatenate([moment, magnetic[None]], axis=0)
    rim = with_halo(stacked, (("gz", 1), ("gy", 2)), 1)
    centre = rim[:, 1:2, 1:-1]
    near = rim[:, 0:1, 1:-1] + rim[:, 2:3, 1:-1] + rim[:, 1:2, :-2] + rim[:, 1:2, 2:]
    padded_x = jnp.pad(centre, ((0, 0), (0, 0), (0, 0), (1, 1)))
    near = near + padded_x[..., :-2] + padded_x[..., 2:]
    exchange = exchange_stiffness * magnetic[None] * (near[:3] - near[3:4] * direction)
    return demag[:, None] + exchange


MESH = pl.DeviceIdType.MESH
most_unrolled_planes = 16


def halves(table):
    high = table.astype(np.float32).astype(jnp.bfloat16)
    low = (table - high.astype(np.float64)).astype(np.float32).astype(jnp.bfloat16)
    return np.stack([high, low])


@functools.lru_cache(maxsize=None)
def tables(columns, rows_total, groups_y, groups_z):
    x = np.arange(columns)
    ang = np.pi / columns * (np.outer(x, x) % (2 * columns))
    c, s = np.cos(ang), np.sin(ang)
    fwd = np.block([[c, -s], [s, c]])
    w = np.where(x == 0, 1.0, 2.0)[:, None]
    inv = np.block([[w * c, w * s], [-w * s, w * c]])
    tx = np.stack([halves(fwd), halves(inv)])
    spec = 2 * rows_total // groups_y
    y = np.arange(rows_total)
    ty = []
    for g in range(groups_y):
        ky = g * spec + np.arange(spec)
        ang = np.pi / rows_total * (np.outer(ky, y) % (2 * rows_total))
        c, s = np.cos(ang), np.sin(ang)
        f = np.block([[c, s], [-s, c]])
        ty.append(np.stack([halves(f), halves(f.T)]))
    ty = np.stack(ty)
    signs = 1.0 - 2.0 * (x % 2)
    gather = np.zeros((6 * columns, columns))
    spread = np.zeros((columns, 6 * columns))
    for b in range(6):
        gather[b * columns : (b + 1) * columns, b] = signs
        gather[b * columns : (b + 1) * columns, b + 6] = signs
        spread[b, b * columns : (b + 1) * columns] = signs
    pick = np.zeros((3, 12, columns))
    for d in range(3):
        for i in range(3):
            for k in range(2):
                pick[d, tensor_index[i][(i + d) % 3] * 2 + k, i * 2 + k] = 1.0
    bits = groups_z.bit_length() - 1
    coef = np.zeros((groups_z, 4 * groups_z))
    plane = np.arange(groups_z)
    for g in range(groups_z):
        rev = sum(((g >> b) & 1) << (bits - 1 - b) for b in range(bits))
        for k in range(2):
            ang = np.pi / groups_z * ((2 * rev + k) * plane % (2 * groups_z))
            coef[g, 2 * k :: 4] = np.cos(ang)
            coef[g, 2 * k + 1 :: 4] = -np.sin(ang)
    return (
        tx,
        ty,
        gather.astype(jnp.bfloat16),
        spread.astype(jnp.bfloat16),
        pick.astype(np.float32),
        coef.astype(np.float32),
    )


def split(value):
    high = value.astype(jnp.bfloat16)
    return high, (value - high.astype(jnp.float32)).astype(jnp.bfloat16)


def mm(a, b):
    return jnp.dot(a, b, preferred_element_type=jnp.float32)


def fused(
    coef,
    sat,
    direction_hbm,
    region_hbm,
    pick_hbm,
    knyq_hbm,
    kmain_hbm,
    tx_hbm,
    ty_hbm,
    gather_hbm,
    spread_hbm,
    out,
    direction,
    region,
    pick,
    knyq,
    mom,
    strength,
    near_strength,
    exch,
    kmain,
    tx,
    ty,
    gather,
    spread,
    zh,
    zl,
    rh,
    rl,
    gh,
    gl,
    afull,
    apeer,
    xsend,
    xrecv,
    upsend,
    uprecv,
    dnsend,
    dnrecv,
    local_sem,
    ag_send,
    ag_ici,
    ag_d2d,
    ag_psend,
    s_send,
    s_recv,
    a_send,
    a_recv,
    x_ssem,
    x_rsem,
    up_ssem,
    up_rsem,
    dn_ssem,
    dn_rsem,
):
    planes = mom.shape[0]
    line = planes // 2
    rows_total = mom.shape[2]
    columns = mom.shape[3]
    rows = direction.shape[2]
    g = lax.axis_index("gz")
    c = lax.axis_index("gy")
    o = g // 2
    xi = g % 2
    side = g + 1 - 2 * xi
    own = pl.ds(pl.multiple_of(c * rows, rows), rows)
    other = pl.ds(pl.multiple_of((1 - c) * rows, rows), rows)
    peer_id = {"gz": g, "gy": 1 - c}
    side_id = {"gz": side, "gy": c}
    up_id = {"gz": g + 2, "gy": c}
    dn_id = {"gz": g - 2, "gy": c}
    after_id = {"gz": g + 1, "gy": c}
    before_id = {"gz": g - 1, "gy": c}
    has_up = o < line - 1
    has_dn = o > 0
    has_after = g < planes - 1
    has_before = g > 0

    barrier = pltpu.get_barrier_semaphore()
    pl.semaphore_signal(barrier, inc=1, device_id=peer_id, device_id_type=MESH)
    pl.semaphore_signal(barrier, inc=1, device_id=side_id, device_id_type=MESH)
    for cond, where in ((has_up, up_id), (has_dn, dn_id), (has_after, after_id), (has_before, before_id)):

        @pl.when(cond)
        def _(where=where):
            pl.semaphore_signal(barrier, inc=1, device_id=where, device_id_type=MESH)

    first = [
        pltpu.make_async_copy(direction_hbm, direction, local_sem.at[5]),
        pltpu.make_async_copy(region_hbm, region, local_sem.at[6]),
    ]
    for copy in first:
        copy.start()
    loads = [
        pltpu.make_async_copy(kmain_hbm, kmain, local_sem.at[0]),
        pltpu.make_async_copy(tx_hbm, tx, local_sem.at[1]),
        pltpu.make_async_copy(ty_hbm.at[c], ty, local_sem.at[2]),
        pltpu.make_async_copy(gather_hbm, gather, local_sem.at[3]),
        pltpu.make_async_copy(spread_hbm, spread, local_sem.at[4]),
        pltpu.make_async_copy(pick_hbm, pick, local_sem.at[7]),
        pltpu.make_async_copy(knyq_hbm, knyq, local_sem.at[8]),
    ]
    for copy in first:
        copy.wait()
    for copy in loads:
        copy.start()

    reg = region[0]
    s = jnp.zeros(reg.shape, jnp.float32)
    for r in range(sat.shape[0]):
        s = s + jnp.where(reg == r + 1, sat[r], 0.0)
    strength[own, :] = s
    for j in range(3):
        mom[g, j, own, :] = direction[j, 0] * s

    friends = 2
    for cond in (has_up, has_dn, has_after, has_before):
        friends = friends + jnp.where(cond, 1, 0)
    pl.semaphore_wait(barrier, friends)

    def chunk_copy(p, j, way):
        where = (up_id, dn_id, side_id)[way]
        block = mom.at[p, j, own, :]
        return pltpu.make_async_remote_copy(
            src_ref=block,
            dst_ref=block,
            send_sem=ag_send.at[way, p, j],
            recv_sem=ag_ici.at[p, j],
            device_id=where,
            device_id_type=MESH,
        )

    def peer_all(half):
        block = mom.at[:, :, half, :]
        return pltpu.make_async_remote_copy(
            src_ref=block,
            dst_ref=block,
            send_sem=ag_psend.at[0],
            recv_sem=ag_d2d.at[0],
            device_id=peer_id,
            device_id_type=MESH,
        )

    def peer_copy(p, j):
        block = mom.at[p, j, own, :]
        return pltpu.make_async_remote_copy(
            src_ref=block,
            dst_ref=block,
            send_sem=ag_psend.at[0],
            recv_sem=ag_d2d.at[0],
            device_id=peer_id,
            device_id_type=MESH,
        )

    def when(cond, action):
        pl.when(cond)(action)

    for j in range(3):
        when(has_up, lambda: chunk_copy(g, j, 0).start())
        when(has_dn, lambda: chunk_copy(g, j, 1).start())
        chunk_copy(g, j, 2).start()

    def strength_copy(way):
        where = (peer_id, after_id, before_id)[way]
        if way == 0:
            dst = strength.at[own, :]
        else:
            dst = near_strength.at[way - 1]
        return pltpu.make_async_remote_copy(
            src_ref=strength.at[own, :],
            dst_ref=dst,
            send_sem=s_send.at[way],
            recv_sem=s_recv.at[way],
            device_id=where,
            device_id_type=MESH,
        )

    for j in range(3):
        peer_copy(g, j).start()

    for h in range(1, line + 1):
        for j in range(3):
            if h < line:

                @pl.when(o >= h)
                def _():
                    p = g - 2 * h
                    chunk_copy(p, j, 2).wait_recv()
                    when(has_up, lambda: chunk_copy(p, j, 0).start())
                    chunk_copy(p, j, 2).start()
                    peer_copy(p, j).start()

                @pl.when(o + h < line)
                def _():
                    p = g + 2 * h
                    chunk_copy(p, j, 2).wait_recv()
                    when(has_dn, lambda: chunk_copy(p, j, 1).start())
                    chunk_copy(p, j, 2).start()
                    peer_copy(p, j).start()

            def side_arrived(p):
                chunk_copy(p, j, 2).wait_recv()
                peer_copy(p, j).start()

            if h == 1:
                side_arrived(side)
            else:
                when(o >= h - 1, lambda: side_arrived(side - 2 * (h - 1)))
                when(o + h - 1 < line, lambda: side_arrived(side + 2 * (h - 1)))

    strength_copy(0).start()
    when(has_after, lambda: strength_copy(1).start())
    when(has_before, lambda: strength_copy(2).start())
    for copy in loads:
        copy.wait()
    peer_all(other).wait_recv()

    step = 32
    for j in range(3):
        for top in range(0, rows_total, step):
            accs = [None] * 4
            for p in range(planes):
                m = mom[p, j, top : top + step, :]
                for q in range(4):
                    term = m * coef[g, 4 * p + q]
                    accs[q] = term if accs[q] is None else accs[q] + term
            for q in range(4):
                hi, lo = split(accs[q])
                at = (2 * j + q // 2) * rows_total + top
                lanes = slice((q % 2) * columns, (q % 2 + 1) * columns)
                zh[at : at + step, lanes] = hi
                zl[at : at + step, lanes] = lo

    nyq = [None, None]
    for b in range(6):
        band = slice(b * rows_total, (b + 1) * rows_total)
        hi, lo = zh[band, :], zl[band, :]
        res = mm(hi, tx[0, 0]) + mm(hi, tx[0, 1]) + mm(lo, tx[0, 0])
        signs = gather[b * columns : (b + 1) * columns, :]
        for q in range(2):
            lanes = slice(q * columns, (q + 1) * columns)
            band_out = slice(q * rows_total, (q + 1) * rows_total)
            cols = slice(b * columns, (b + 1) * columns)
            rhi, rlo = split(res[:, lanes])
            rh[band_out, cols] = rhi
            rl[band_out, cols] = rlo
            n = mm(hi[:, lanes], signs) + mm(lo[:, lanes], signs)
            nyq[q] = n if nyq[q] is None else nyq[q] + n
    nyq_cols = slice(6 * columns, 7 * columns)
    for q in range(2):
        band_out = slice(q * rows_total, (q + 1) * rows_total)
        rhi, rlo = split(nyq[q])
        rh[band_out, nyq_cols] = rhi
        rl[band_out, nyq_cols] = rlo

    spec = kmain.shape[2]

    def column_pass(t, b):
        cols = slice(b * columns, (b + 1) * columns)
        hi, lo = (rh, rl) if t == 0 else (gh, gl)
        hi, lo = hi[:, cols], lo[:, cols]
        return mm(ty[t, 0], hi) + mm(ty[t, 1], hi) + mm(ty[t, 0], lo)

    for k in range(2):
        spectra = [column_pass(0, 2 * j + k) for j in range(3)]
        for i in range(3):
            cols = slice((2 * i + k) * columns, (2 * i + k + 1) * columns)
            for q in range(2):
                band = slice(q * spec, (q + 1) * spec)
                total = kmain[tensor_index[i][0], k] * spectra[0][band]
                for j in (1, 2):
                    total = total + kmain[tensor_index[i][j], k] * spectra[j][band]
                hi, lo = split(total)
                gh[band, cols] = hi
                gl[band, cols] = lo
    spectrum = column_pass(0, 6)
    factors = knyq[...].reshape(12, spec)
    totals = [None, None]
    for d in range(3):
        factor = lax.dot_general(
            factors, pick[d], (((0,), (0,)), ((), ())), precision=highest, preferred_element_type=jnp.float32
        )
        moved = spectrum if d == 0 else pltpu.roll(spectrum, columns - 2 * d, 1)
        for q in range(2):
            term = factor * moved[q * spec : (q + 1) * spec]
            totals[q] = term if totals[q] is None else totals[q] + term
    for q in range(2):
        hi, lo = split(totals[q])
        gh[q * spec : (q + 1) * spec, nyq_cols] = hi
        gl[q * spec : (q + 1) * spec, nyq_cols] = lo

    back = column_pass(1, 6)
    nyq_back = [split(back[:rows_total]), split(back[rows_total:])]

    def a_copy(j):
        return pltpu.make_async_remote_copy(
            src_ref=afull.at[j, :, other, :],
            dst_ref=apeer.at[j],
            send_sem=a_send.at[j],
            recv_sem=a_recv.at[j],
            device_id=peer_id,
            device_id_type=MESH,
        )

    for j in range(3):
        for k in range(2):
            b = 2 * j + k
            back = column_pass(1, b)
            parts = [split(back[:rows_total]), split(back[rows_total:])]
            hi = jnp.concatenate([parts[0][0], parts[1][0]], axis=1)
            lo = jnp.concatenate([parts[0][1], parts[1][1]], axis=1)
            res = mm(hi, tx[1, 0]) + mm(hi, tx[1, 1]) + mm(lo, tx[1, 0])
            signs = spread[:, b * columns : (b + 1) * columns]
            for q in range(2):
                extra = mm(nyq_back[q][0], signs) + mm(nyq_back[q][1], signs)
                afull[j, 2 * k + q] = res[:, q * columns : (q + 1) * columns] + extra
        a_copy(j).start()

    def contribution(p, j):
        total = None
        for q in range(4):
            term = apeer[j, q] * coef[g, 4 * p + q]
            total = term if total is None else total + term
        return total

    def rs_copy(d, j, way):
        src, dst, ssem, rsem, where = (
            (xsend, xrecv, x_ssem, x_rsem, side_id),
            (upsend, uprecv, up_ssem, up_rsem, up_id),
            (dnsend, dnrecv, dn_ssem, dn_rsem, dn_id),
        )[way]
        return pltpu.make_async_remote_copy(
            src_ref=src.at[d, j],
            dst_ref=dst.at[d, j],
            send_sem=ssem.at[d, j],
            recv_sem=rsem.at[d, j],
            device_id=where,
            device_id_type=MESH,
        )

    def side_send(d, j):
        xsend[d, j] = contribution(2 * d + 1 - xi, j)
        rs_copy(d, j, 0).start()

    for j in range(3):
        a_copy(j).wait_recv()
        for q in range(4):
            apeer[j, q] = apeer[j, q] + afull[j, q, own, :]
        when(o + line - 1 < line, lambda: side_send(o + line - 1, j))
        when(o - line + 1 >= 0, lambda: side_send(o - line + 1, j))
    for h in range(line - 2, -1, -1):
        for j in range(3):
            if h == 0:
                side_send(o, j)
            else:
                when(o + h < line, lambda: side_send(o + h, j))
                when(o - h >= 0, lambda: side_send(o - h, j))

    def exchange():
        strength_copy(0).wait_recv()
        for way, cond in ((1, has_before), (2, has_after)):

            @pl.when(cond)
            def _(way=way):
                strength_copy(way).wait_recv()

            @pl.when(jnp.logical_not(cond))
            def _(way=way):
                near_strength[way - 1] = jnp.zeros(near_strength.shape[1:], jnp.float32)

        full = strength[...]
        inverse = jnp.where(full > 0, 1.0 / jnp.where(full > 0, full, 1.0), 0.0)
        present = jnp.where(full > 0, 1.0, 0.0)
        row_id = lax.broadcasted_iota(jnp.int32, full.shape, 0)
        col_id = lax.broadcasted_iota(jnp.int32, full.shape, 1)

        def plane_near(v):
            total = jnp.where(row_id > 0, pltpu.roll(v, 1, 0), 0.0)
            total = total + jnp.where(row_id < rows_total - 1, pltpu.roll(v, rows_total - 1, 0), 0.0)
            total = total + jnp.where(col_id > 0, pltpu.roll(v, 1, 1), 0.0)
            return total + jnp.where(col_id < columns - 1, pltpu.roll(v, columns - 1, 1), 0.0)

        for j in range(3):
            exch[j] = plane_near(mom[g, j] * inverse)
        exch[3] = plane_near(present)
        adjacent = []
        for way in range(2):
            near_s = near_strength[way]
            there = near_s > 0
            adjacent.append(
                (jnp.where(there, 1.0 / jnp.where(there, near_s, 1.0), 0.0), jnp.where(there, 1.0, 0.0))
            )
        count = exch[3, own, :] + adjacent[0][1] + adjacent[1][1]
        mask = jnp.where(region[0] > 0, exchange_stiffness, 0.0)
        lower = jnp.maximum(g - 1, 0)
        upper = jnp.minimum(g + 1, planes - 1)
        for j in range(3):
            near = exch[j, own, :] + mom[lower, j, own, :] * adjacent[0][0]
            near = near + mom[upper, j, own, :] * adjacent[1][0]
            out[j, 0] = mask * (near - count * direction[j, 0])

    for h in range(line - 1, 0, -1):
        for j in range(3):

            def hop(d, way, cond):
                stage, arrived = ((upsend, uprecv), (dnsend, dnrecv))[way - 1]
                rs_copy(d, j, 0).wait_recv()
                stage[d, j] = contribution(2 * d + xi, j) + xrecv[d, j]

                @pl.when(cond)
                def _():
                    rs_copy(d, j, way).wait_recv()
                    stage[d, j] = stage[d, j] + arrived[d, j]

                rs_copy(d, j, way).start()

            when(o + h < line, lambda: hop(o + h, 1, has_dn))
            when(o - h >= 0, lambda: hop(o - h, 2, has_up))
        if h == line - 1:
            exchange()

    scale = 1.0 / (4 * rows_total * columns * 2 * planes)
    for j in range(3):
        rs_copy(o, j, 0).wait_recv()
        exch[j, :rows, :] = contribution(g, j) + xrecv[o, j]

        @pl.when(has_dn)
        def _():
            rs_copy(o, j, 1).wait_recv()
            exch[j, :rows, :] = exch[j, :rows, :] + uprecv[o, j]

        @pl.when(has_up)
        def _():
            rs_copy(o, j, 2).wait_recv()
            exch[j, :rows, :] = exch[j, :rows, :] + dnrecv[o, j]

        out[j, 0] = out[j, 0] + exch[j, :rows, :] * scale

    peer_all(own).wait_send()
    strength_copy(0).wait_send()
    when(has_after, lambda: strength_copy(1).wait_send())
    when(has_before, lambda: strength_copy(2).wait_send())
    for j in range(3):
        a_copy(j).wait_send()
        for d in range(line):
            chunk_copy(2 * d + xi, j, 2).wait_send()
            rs_copy(d, j, 0).wait_send()

            @pl.when(jnp.logical_and(has_up, o >= d))
            def _():
                chunk_copy(2 * d + xi, j, 0).wait_send()

            @pl.when(jnp.logical_and(has_dn, o <= d))
            def _():
                chunk_copy(2 * d + xi, j, 1).wait_send()

            when(o < d, lambda: rs_copy(d, j, 1).wait_send())
            when(o > d, lambda: rs_copy(d, j, 2).wait_send())


def fused_local(direction, region, saturation, kernel_main, kernel_nyq):
    rows, columns = direction.shape[2:]
    planes = lax.axis_size("gz")
    groups_y = lax.axis_size("gy")
    rows_total = rows * groups_y
    spec = kernel_main.shape[2]
    line = planes // 2
    tx, ty, gather, spread, pick, coef = (
        jnp.asarray(t) for t in tables(columns, rows_total, groups_y, planes)
    )
    f32, bf16 = jnp.float32, jnp.bfloat16
    vmem = pl.BlockSpec(memory_space=pltpu.VMEM)
    smem = pl.BlockSpec(memory_space=pltpu.SMEM)
    hbm = pl.BlockSpec(memory_space=pltpu.HBM)
    dma = pltpu.SemaphoreType.DMA
    stage = pltpu.VMEM((line, 3, rows, columns), f32)
    return pl.pallas_call(
        fused,
        out_shape=jax.ShapeDtypeStruct(direction.shape, f32),
        in_specs=[smem, smem, hbm, hbm, hbm, hbm, hbm, hbm, hbm, hbm, hbm],
        out_specs=vmem,
        scratch_shapes=[
            pltpu.VMEM(direction.shape, f32),
            pltpu.VMEM(region.shape, jnp.int32),
            pltpu.VMEM(pick.shape, f32),
            pltpu.VMEM(kernel_nyq.shape, f32),
            pltpu.VMEM((planes, 3, rows_total, columns), f32),
            pltpu.VMEM((rows_total, columns), f32),
            pltpu.VMEM((2, rows, columns), f32),
            pltpu.VMEM((4, rows_total, columns), f32),
            pltpu.VMEM(kernel_main.shape, f32),
            pltpu.VMEM(tx.shape, bf16),
            pltpu.VMEM(ty.shape[1:], bf16),
            pltpu.VMEM(gather.shape, bf16),
            pltpu.VMEM(spread.shape, bf16),
            pltpu.VMEM((6 * rows_total, 2 * columns), bf16),
            pltpu.VMEM((6 * rows_total, 2 * columns), bf16),
            pltpu.VMEM((2 * rows_total, 7 * columns), bf16),
            pltpu.VMEM((2 * rows_total, 7 * columns), bf16),
            pltpu.VMEM((2 * spec, 7 * columns), bf16),
            pltpu.VMEM((2 * spec, 7 * columns), bf16),
            pltpu.VMEM((3, 4, rows_total, columns), f32),
            pltpu.VMEM((3, 4, rows, columns), f32),
            stage,
            stage,
            stage,
            stage,
            stage,
            stage,
            dma((9,)),
            dma((3, planes, 3)),
            dma((planes, 3)),
            dma((1,)),
            dma((1,)),
            dma((3,)),
            dma((3,)),
            dma((3,)),
            dma((3,)),
            dma((line, 3)),
            dma((line, 3)),
            dma((line, 3)),
            dma((line, 3)),
            dma((line, 3)),
            dma((line, 3)),
        ],
        compiler_params=pltpu.CompilerParams(
            collective_id=0, has_side_effects=True, vmem_limit_bytes=67043328
        ),
        name="field_kernel",
    )(coef, saturation, direction, region, pick, kernel_nyq, kernel_main, tx, ty, gather, spread)


def solution(mesh):
    placed = (
        P(None, ("parts", "gz"), "gy", None),
        P(("parts", "gz"), "gy", None),
        P(),
        P(None, "gz", "gy", None),
        P(None, "gz", "gy"),
    )
    small = mesh.shape["gz"] <= most_unrolled_planes and mesh.shape["gy"] == 2
    return jax.shard_map(
        fused_local if small else local,
        mesh=mesh,
        in_specs=placed,
        out_specs=P(None, ("parts", "gz"), "gy", None),
        check_vma=False,
    )
```
